32 devices in a mesh: grp: 2 (over y), exp: 4 (over z), tp: 4 (over x, core).
Axes of the slice: x: 2, y: 2, z: 4, core: 2. Of those that a mesh axis runs over, the one named last changes fastest.
Arguments:
- tokens: bfloat16 [128, 3584], P(('grp', 'exp'), 'tp'), parts along dimension 0, may hold values from -6 to 6
- gate_up_weight: bfloat16 [3584, 2, 18944], P('tp', None, 'exp'), may hold values from -0.09375 to 0.09375
- down_weight: bfloat16 [18944, 3584], P('exp', 'tp'), may hold values from -0.046875 to 0.046875
- adapter_in: bfloat16 [4, 3584, 16], P('exp', 'tp'), may hold values from -0.09375 to 0.09375
- adapter_out: bfloat16 [4, 16, 3584], P('exp', None, 'tp'), may hold values from -1.5 to 1.5
- expert_ids: int32 [128, 2], P(('grp', 'exp')), parts along dimension 0, may hold values from 0 to 3, all different within a row; in each aligned block of 16 rows (0 to 15, 16 to 31, ...) at most 16 rows name the same one
- route_weight: float32 [128, 2], P(('grp', 'exp')), parts along dimension 0, may hold values from 0.2 to 1
Outputs:
- mixed: bfloat16 [128, 3584], P(('grp', 'exp'), 'tp'), parts along dimension 0
The draws below stay inside these ranges and needn't reach their ends.
There are 2 independent parts, one for each index of `grp`. The reference program is written for one: setup_inputs(seed, part) draws one part's arguments, and reference() takes and returns one part's arrays. A program takes and returns all parts, laid end to end along the dimension named above; an argument that names none is the same for every part. Nothing has to cross between parts.
Inputs may be any that keep to these rules, and one draw needn't show every extreme that they name: `expert_ids`: each row names 2 different experts. Among the 16 rows of one index of exp (aligned blocks of 16 rows) no expert is named by more than 16 rows, and in every draw some expert is named by exactly 16 rows of some block.
All inputs are finite; a program needn't handle non-finite values.
Results may differ from the reference program's by a relative error of at most 0.025.
Values may be sent and summed in bfloat16 or wider, within the bound.
A program may use at most 64 MiB of HBM per device.

```python
import math
import jax
import jax.numpy as jnp
import numpy as np
from jax import lax

D = 3584
FF = 18944
RANK = 16
TOP = 2
TOK_DEV = 16
EXPERTS = 4
TOKENS = 64
CAP = 16
N_EXP = 4
N_TP = 4


def steps_of(key, dims, cuts, least, top_value):
    level, own = 1.0, jax.random.fold_in(key, 6)
    for dim, shards_of in cuts:
        heights = jnp.exp(jax.random.uniform(jax.random.fold_in(own, dim), (shards_of,), jnp.float32, least / len(cuts), top_value / len(cuts)))
        level = level * jnp.repeat(heights, dims[dim] // shards_of).reshape([-1 if axis == dim else 1 for axis in range(len(dims))])
    return level


def assign_block(key, own, number, rows, count, top, reach, skew):
    sequence = jax.random.permutation(key, count)
    crowded, common = portions_of(count, rows * top, reach, skew, True), portions_of(count, rows * top, reach, skew, False)
    places = jnp.arange(count)

    def named(lengths, turn):
        used = int((lengths > 0).sum())
        fixed = max(1, used // 4)
        shifted = fixed + (places - fixed + turn * (used - fixed)) % max(1, count - fixed)
        return jnp.zeros((count,), jnp.int32).at[sequence[jnp.where(places < fixed, places, shifted)]].set(jnp.asarray(lengths, jnp.int32))

    lengths = jnp.where(number % 4 == 0, named(crowded, number // 4), named(common, number - number // 4 - 1))
    mixed = jax.random.permutation(jax.random.fold_in(own, 3), count)
    donor, taker = mixed[0:count // 2 * 2:2], mixed[1:count // 2 * 2:2]
    margin = jnp.minimum(lengths[donor] - 1, reach - lengths[taker]) // 2
    margin = jnp.where((donor == sequence[0]) | (taker == sequence[0]) | (lengths[taker] == 0), 0, jnp.maximum(margin, 0))
    shifted = jax.random.randint(jax.random.fold_in(own, 4), (count // 2,), 0, 1 << 20) % (margin + 1)
    lengths = lengths.at[donor].add(-shifted).at[taker].add(shifted)
    members = jnp.searchsorted(jnp.cumsum(lengths), jnp.arange(rows * top), side="right").astype(jnp.int32)
    listing = members.reshape(top, rows).T
    listing = listing[jax.random.permutation(jax.random.fold_in(own, 1), rows)]
    turn = jax.random.randint(jax.random.fold_in(own, 2), (rows, 1), 0, top)
    return jnp.take_along_axis(listing, (jnp.arange(top)[None, :] + turn) % top, axis=1)


def portions_of(count, total, bound, slope, full):
    portions = [(1 << 20) // math.isqrt(rank ** slope) + 1 for rank in range(1, count + 1)]
    largest = bound if full else min(bound, max(-(-total // count), total * portions[0] // sum(portions)))
    least = 1 if total - largest >= count - 1 else 0
    holding, spare = [largest] + [least] * (count - 1), total - largest - least * (count - 1)
    while spare > 0:
        candidates = [i for i in range(1, count) if holding[i] < largest] or [i for i in range(1, count) if holding[i] < bound]
        whole, remaining = sum([portions[i] for i in candidates]), spare
        for i in candidates:
            more = min(bound - holding[i], max(1, remaining * portions[i] // whole), spare)
            holding[i] = holding[i] + more
            spare = spare - more
    return np.array(holding)


def scatter_about(own_key, shape, width, most, cuts=(), kind=jnp.bfloat16):
    level = steps_of(own_key, shape, cuts, -0.22, 0.18) if cuts else 1.0
    result = jax.random.normal(own_key, shape, jnp.float32) * width * level
    return jnp.minimum(jnp.maximum(result, -most), most).astype(kind)


def setup_inputs(seed: int = 0, part: int = 0) -> dict:
    keys = jax.random.split(jax.random.key(seed), 8)
    part_splits = jax.random.split(jax.random.fold_in(keys[7], part), 8)
    tokens = scatter_about(part_splits[0], (TOKENS, D), 1.0, 6.0, ((0, 4), (1, 4)))
    gate_up_weight = scatter_about(keys[1], (D, 2, FF), D ** -0.5, 0.09375, ((0, 4), (2, 4)))
    down_weight = scatter_about(keys[2], (FF, D), FF ** -0.5, 0.046875, ((0, 4), (1, 4)))
    adapter_in = scatter_about(keys[3], (EXPERTS, D, RANK), D ** -0.5, 0.09375, ((0, 4), (1, 4)))
    adapter_out = scatter_about(keys[4], (EXPERTS, RANK, D), RANK ** -0.5, 1.5, ((0, 4), (2, 4)))
    expert_ids_keys = jax.random.split(jax.random.fold_in(part_splits[5], 1), TOKENS // TOK_DEV)
    expert_ids_turns = jax.random.permutation(jax.random.fold_in(part_splits[5], 3), TOKENS // TOK_DEV)
    expert_ids = jax.vmap(lambda own, number: assign_block(jax.random.fold_in(part_splits[5], 2), own, number, TOK_DEV, EXPERTS, TOP, CAP, 2))(expert_ids_keys, expert_ids_turns).reshape((TOKENS, TOP))
    route_weight = jnp.clip(0.2 + 0.8 * jax.random.uniform(part_splits[6], (TOKENS, TOP), jnp.float32) ** steps_of(part_splits[6], (TOKENS, TOP), ((0, 4),), -0.2, 0.2), 0.2, 1.0)
    return dict(tokens=tokens, gate_up_weight=gate_up_weight, down_weight=down_weight, adapter_in=adapter_in, adapter_out=adapter_out, expert_ids=expert_ids, route_weight=route_weight)


def reference(tokens, gate_up_weight, down_weight, adapter_in, adapter_out, expert_ids, route_weight):
    token_count = tokens.shape[0]
    feat_width = D // N_TP
    pair = jnp.zeros((token_count, 2 * FF), jnp.float32)
    for block_index in range(N_TP):
        lower = block_index * feat_width
        block_weight = gate_up_weight[lower:lower + feat_width].reshape(feat_width, 2 * FF)
        partial_sum = jnp.dot(tokens[:, lower:lower + feat_width], block_weight, preferred_element_type=jnp.float32)
        rounded = lax.optimization_barrier(partial_sum.astype(jnp.bfloat16))
        pair = pair + rounded.astype(jnp.float32)
    gate = pair[:, :FF]
    up_part = pair[:, FF:]
    hidden = (jax.nn.silu(gate) * up_part).astype(jnp.bfloat16)
    hidden_width = FF // N_EXP
    base_out = jnp.zeros((token_count, D), jnp.float32)
    for block_index in range(N_EXP):
        lower = block_index * hidden_width
        partial_sum = jnp.dot(hidden[:, lower:lower + hidden_width], down_weight[lower:lower + hidden_width], preferred_element_type=jnp.float32)
        rounded = lax.optimization_barrier(partial_sum.astype(jnp.bfloat16))
        base_out = base_out + rounded.astype(jnp.float32)
    expert_count = adapter_in.shape[0]
    in_flat = jnp.transpose(adapter_in, (1, 0, 2)).reshape(D, expert_count * RANK)
    rank_mid = jnp.dot(tokens, in_flat, preferred_element_type=jnp.float32).astype(jnp.bfloat16)
    rank_mid = rank_mid.reshape(token_count, expert_count, RANK)
    hits = (expert_ids[:, :, None] == jnp.arange(expert_count, dtype=jnp.int32)[None, None, :]).astype(jnp.float32)
    coefficient = jnp.sum(hits * route_weight[:, :, None], axis=1)

    def add_expert(total, pieces):
        mid_piece, out_map, coef_column = pieces
        expert_out = jnp.dot(mid_piece, out_map, preferred_element_type=jnp.float32).astype(jnp.bfloat16)
        return total + coef_column[:, None] * expert_out.astype(jnp.float32), None

    adapter_sum, _ = lax.scan(add_expert, jnp.zeros((token_count, D), jnp.float32),
                              (jnp.transpose(rank_mid, (1, 0, 2)), adapter_out, coefficient.T))
    return (base_out + adapter_sum).astype(jnp.bfloat16)
```

```python
import functools
import jax
import jax.numpy as jnp
from jax import lax
from jax.experimental import pallas as pl
from jax.experimental.pallas import tpu as pltpu
from jax.sharding import PartitionSpec as P

LANES = 128
CHUNK_TILES = 6
EARLY_CHUNKS = 3
MESH = pl.DeviceIdType.MESH
BF16, F32 = jnp.bfloat16, jnp.float32
NEAR, FAR = 0, 1

NEAR_READY, FAR_READY = 4.2, 6.0
LOAD_START, LOAD_TILE = 0.9, 0.135
DOT_BASE, DOT_TILE = 0.15, 0.083
DOWN_BASE, DOWN_TILE = 0.12, 0.04
PARTNER_DELAY, ACROSS_DELAY = 1.05, 2.3
ACROSS_HALF_TILE = 0.088


def chunks_of(columns):
    spans, first = [], 0
    while first < columns:
        count = min(CHUNK_TILES, columns - first)
        spans.append((first, count))
        first += count
    return spans


def plan(spans):
    count = len(spans)
    early = min(EARLY_CHUNKS, count)
    rank = {}
    for s, chunks in ((NEAR, range(early)), (FAR, range(count)), (NEAR, range(early, count))):
        for j in chunks:
            rank[s, j] = len(rank)
    products = [((NEAR,), j) for j in range(early)] + [((FAR,), j) for j in range(early)]
    products += [((FAR, NEAR), j) for j in range(early, count)]
    ready = {}
    pending_down = [((NEAR, FAR), j) for j in range(early)]
    pending_down += [((FAR,), j) for j in range(early, count)]
    pending_down += [((NEAR,), j) for j in range(early, count)]
    now, link, order = 0.0, 0.0, []
    loaded = lambda j: LOAD_START + LOAD_TILE * (spans[j][0] + spans[j][1])
    waiting = []

    def send(j, tiles_half):
        nonlocal link
        link = max(link, now) + ACROSS_HALF_TILE * tiles_half
        return link + ACROSS_DELAY

    far_left = count
    near_left = count
    while products or waiting or pending_down:
        options = []
        for name, s, j in waiting:
            options.append((ready[name, s, j], (0 if name != "relay" else 1, rank[s, j]), (name, s, j)))
        if products:
            sets, j = products[0]
            at = max(loaded(j), max(NEAR_READY if s == NEAR else FAR_READY for s in sets))
            options.append((at, (2, 0), ("product", sets, j)))
        for sets, j in pending_down:
            at = [ready.get(("project", s, j)) for s in sets]
            if None not in at:
                place = 3 if sets != (FAR,) else 2
                options.append((max(at), (place, rank[sets[-1], j]), ("project", sets, j)))
        able = [o for o in options if o[0] <= now + 0.02]
        pick = min(able, key=lambda o: o[1]) if able else min(options)
        now = max(now, pick[0])
        name, s, j = pick[2]
        order.append(pick[2])
        half = spans[j][1] / 2
        if name == "product":
            products.pop(0)
            now += DOT_BASE + DOT_TILE * spans[j][1]
            for one in s:
                waiting.append(("reduce", one, j))
                ready["reduce", one, j] = now + PARTNER_DELAY
        elif name == "project":
            pending_down.remove((s, j))
            now += DOWN_BASE + DOWN_TILE * spans[j][1]
            if FAR in s:
                far_left -= 1
                if far_left == 0:
                    order.append(("finish", FAR, 0))
            if NEAR in s:
                near_left -= 1
                if near_left == 0:
                    order.append(("finish", NEAR, 0))
        else:
            waiting.remove(pick[2])
            now += 0.03
            if name == "reduce":
                waiting.append(("activate", s, j))
                ready["activate", s, j] = send(j, 2 * half)
            elif name == "activate":
                waiting.append(("relay", s, j))
                ready["relay", s, j] = send(j, half)
            else:
                ready["project", s, j] = now + PARTNER_DELAY
    return order


def kernel(
    tok_ref, gu_ref, down_ref, ain_ref, aout_ref, ids_ref, weight_ref, out_ref,
    gu, down, tok_all, ain_pad, aout_pad, ids, weights, coef_own, coef_all, lhs,
    keep1, send1, recv1, keep2, send2, recv2, hid, total, send_f, recv_f,
    gu_sem, down_sem, in_sem, tok_send, tok_recv, coef_send, coef_recv,
    s1_send, s1_recv, s2_send, s2_recv, hp_send, hp_recv, hx_send, hx_recv, hr_send, hr_recv,
    f_send, f_recv,
):
    me = lax.axis_index("exp")
    tp = lax.axis_index("tp")
    own_rows, feat = tok_ref.shape
    hidden = gu_ref.shape[2]
    rank = ain_ref.shape[1]
    tiles = hidden // LANES
    spans = chunks_of(tiles + 1)
    core, side = tp % 2, tp // 2
    partner = side * 2 + (1 - core)
    across = (1 - side) * 2 + core
    low = me - me % 2
    lows = (low, (low + 2) % 4)
    near = low + 1 - me % 2
    far = (me + 2) % 4
    peers = (near, far, (near + 2) % 4)

    barrier = pltpu.get_barrier_semaphore()
    for peer in peers:
        pl.semaphore_signal(barrier, inc=1, device_id={"exp": peer}, device_id_type=MESH)
    for peer in (partner, across):
        pl.semaphore_signal(barrier, inc=1, device_id={"tp": peer}, device_id_type=MESH)

    in_copies = [
        pltpu.make_async_copy(tok_ref, tok_all.at[me], in_sem.at[0]),
        pltpu.make_async_copy(ids_ref, ids, in_sem.at[1]),
        pltpu.make_async_copy(weight_ref, weights, in_sem.at[2]),
        pltpu.make_async_copy(ain_ref.at[0], ain_pad.at[pl.ds(0, rank)], in_sem.at[3]),
        pltpu.make_async_copy(aout_ref.at[0], aout_pad.at[pl.ds(0, rank)], in_sem.at[4]),
    ]
    gu_flat = gu_ref.reshape(2 * feat, hidden)

    def gu_copy(t):
        cols = pl.ds(pl.multiple_of(t * LANES, LANES), LANES)
        return pltpu.make_async_copy(gu_flat.at[:, cols], gu.at[t], gu_sem.at[t])

    def down_rows(j):
        first, count = spans[j]
        begin, end = max(first - 1, 0), first + count - 1
        return pl.ds(begin * LANES, (end - begin) * LANES)

    def down_copy(j):
        rows = down_rows(j)
        return pltpu.make_async_copy(down_ref.at[rows], down.at[rows], down_sem.at[j])

    for copy in in_copies:
        copy.start()

    def start_gu(t, carry):
        gu_copy(t).start()
        return carry

    lax.fori_loop(0, tiles, start_gu, 0)
    for j in range(len(spans)):
        down_copy(j).start()

    ain_pad[rank:, :] = jnp.zeros((LANES - rank, feat), BF16)
    aout_pad[rank:, :] = jnp.zeros((LANES - rank, feat), BF16)

    def exp_copy(src, dst, send, recv, r):
        return pltpu.make_async_remote_copy(
            src_ref=src, dst_ref=dst, send_sem=send.at[r], recv_sem=recv.at[r],
            device_id={"exp": peers[r]}, device_id_type=MESH,
        )

    tok_copies = [
        exp_copy(tok_all.at[me], tok_all.at[me], tok_send, tok_recv, r) for r in range(3)
    ]
    coef_copies = [
        exp_copy(coef_own.at[r], coef_all.at[me], coef_send, coef_recv, r) for r in range(3)
    ]
    in_copies[1].wait()
    in_copies[2].wait()

    def coef_line(expert):
        line = jnp.zeros((1, own_rows), F32)
        for k in range(ids.shape[0]):
            line = line + jnp.where(ids[k:k + 1, :] == expert, weights[k:k + 1, :], 0.0)
        return jnp.concatenate([line, jnp.zeros((1, LANES - own_rows), F32)], axis=1)

    for r in range(3):
        coef_own[r, 0:1, :] = coef_line(peers[r])
    coef_all[me, 0:1, :] = coef_line(me)
    in_copies[0].wait()

    pl.semaphore_wait(barrier, 5)
    for copy in tok_copies + coef_copies:
        copy.start()

    def span_cols(j):
        first, count = spans[j]
        return pl.ds(first * LANES, count * LANES)

    def half_cols(j, which):
        first, count = spans[j]
        width = count // 2 * LANES
        return pl.ds(pl.multiple_of(first * LANES + which * width, LANES), width)

    def pack_cols(j):
        first, count = spans[j]
        return pl.ds(first // 2 * LANES, count // 2 * LANES)

    def tp_copy(src, dst, send, recv, s, j, peer):
        return pltpu.make_async_remote_copy(
            src_ref=src, dst_ref=dst, send_sem=send.at[s, j], recv_sem=recv.at[s, j],
            device_id={"tp": peer}, device_id_type=MESH,
        )

    def s1_copy(s, j):
        cols = span_cols(j)
        return tp_copy(
            send1.at[s, :, cols], recv1.at[s, :, cols], s1_send, s1_recv, s, j, partner
        )

    def s2_copy(s, j):
        cols = pack_cols(j)
        return tp_copy(
            send2.at[s, :, cols], recv2.at[s, :, cols], s2_send, s2_recv, s, j, across
        )

    def hp_copy(s, j):
        ref = hid.at[s, core, :, half_cols(j, side)]
        return tp_copy(ref, ref, hp_send, hp_recv, s, j, partner)

    def hx_copy(s, j):
        ref = hid.at[s, core, :, half_cols(j, side)]
        return tp_copy(ref, ref, hx_send, hx_recv, s, j, across)

    def hr_copy(s, j):
        ref = hid.at[s, core, :, half_cols(j, 1 - side)]
        return tp_copy(ref, ref, hr_send, hr_recv, s, j, partner)

    pair_rows = 2 * own_rows
    row = lax.broadcasted_iota(jnp.int32, (LANES, 4 * LANES), 0)
    col = lax.broadcasted_iota(jnp.int32, (LANES, 4 * LANES), 1)
    spread = jnp.where(col % (2 * LANES) == 2 * row + col // (2 * LANES), 1.0, 0.0).astype(BF16)

    def ordered(s):
        return jnp.concatenate([tok_all[lows[s] + core], tok_all[lows[s] + 1 - core]], axis=0)

    def prepare(s):
        for r in ((0,) if s == NEAR else (1, 2)):
            tok_copies[r].wait_recv()
        tokens = ordered(s)
        stacked = jnp.concatenate(
            [tokens[:, k * LANES:(k + 1) * LANES] for k in range(feat // LANES)], axis=0
        )
        wide = jnp.dot(stacked, spread, preferred_element_type=F32).astype(BF16)
        for k in range(feat // LANES):
            for p in range(2):
                for half in range(2):
                    to = 2 * s * pair_rows + (2 * p + half) * own_rows
                    lhs[to:to + own_rows, 2 * k * LANES:2 * (k + 1) * LANES] = wide[
                        k * pair_rows + p * own_rows:k * pair_rows + (p + 1) * own_rows,
                        2 * half * LANES:2 * (half + 1) * LANES,
                    ]
        if s == NEAR:
            in_copies[3].wait()
        value = lax.dot_general(
            tokens, ain_pad[...], (((1,), (1,)), ((), ())), preferred_element_type=F32
        )
        blank = jnp.zeros((own_rows, LANES), F32)
        store_pair(
            s, pl.ds(0, LANES),
            jnp.concatenate([value[:own_rows], blank, value[own_rows:], blank], axis=0),
        )

    def store_pair(s, cols, value):
        keep1[s, :, cols] = value[:pair_rows]
        send1[s, :, cols] = value[pair_rows:].astype(BF16)

    arrived = set()

    def product(sets, j):
        for s in sets:
            if s not in arrived:
                arrived.add(s)
                prepare(s)
        first, count = spans[j]
        begin, end = max(first - 1, 0), first + count - 1
        for t in range(begin, end):
            if ("gu", t) not in arrived:
                arrived.add(("gu", t))
                gu_copy(t).wait()
        weight = jnp.concatenate([gu[t] for t in range(begin, end)], axis=1)
        rows = slice(0, 4 * pair_rows) if len(sets) == 2 else slice(
            2 * sets[0] * pair_rows, 2 * (sets[0] + 1) * pair_rows
        )
        value = jnp.dot(lhs[rows, :], weight, preferred_element_type=F32)
        cols = pl.ds((begin + 1) * LANES, (end - begin) * LANES)
        for s in sets:
            at = 2 * s * pair_rows if len(sets) == 2 else 0
            store_pair(s, cols, value[at:at + 2 * pair_rows])
            s1_copy(s, j).start()

    def reduce(s, j):
        s1_copy(s, j).wait_recv()
        cols = pack_cols(j)
        kept, sent = half_cols(j, side), half_cols(j, 1 - side)
        send2[s, :, cols] = (keep1[s, :, sent] + recv1[s, :, sent].astype(F32)).astype(BF16)
        s2_copy(s, j).start()
        keep2[s, :, cols] = keep1[s, :, kept] + recv1[s, :, kept].astype(F32)

    def activate(s, j):
        s2_copy(s, j).wait_recv()
        cols = pack_cols(j)
        pair = keep2[s, :, cols] + recv2[s, :, cols].astype(F32)
        value = jax.nn.silu(pair[:own_rows]) * pair[own_rows:]
        if j == 0:
            first = jnp.where(side == 0, pair[:own_rows, :LANES], value[:, :LANES])
            value = jnp.concatenate([first, value[:, LANES:]], axis=1)
        hid[s, core, :, half_cols(j, side)] = value.astype(BF16)
        hx_copy(s, j).start()
        hp_copy(s, j).start()

    def relay(s, j):
        hx_copy(s, j).wait_recv()
        hr_copy(s, j).start()

    diagonal = lax.broadcasted_iota(
        jnp.int32, (own_rows, own_rows), 0
    ) == lax.broadcasted_iota(jnp.int32, (own_rows, own_rows), 1)

    def adapter_part(s):
        if s == NEAR:
            in_copies[4].wait()
        for r in ((0,) if s == NEAR else (1, 2)):
            coef_copies[r].wait_recv()
        rank_mid = hid[s, :, :, pl.ds(0, LANES)].reshape(pair_rows, LANES)
        expert_out = jnp.dot(rank_mid, aout_pad[...], preferred_element_type=F32).astype(BF16)
        columns = []
        for c in range(2):
            line = coef_all[lows[s] + c, 0:1, :][:, :own_rows]
            columns.append(jnp.sum(jnp.where(diagonal, line, 0.0), axis=1, keepdims=True))
        return jnp.concatenate(columns, axis=0) * expert_out.astype(F32)

    def project(sets, j):
        for s in sets:
            hp_copy(s, j).wait_recv()
            hr_copy(s, j).wait_recv()
        if ("down", j) not in arrived:
            arrived.add(("down", j))
            down_copy(j).wait()
        first, count = spans[j]
        begin, end = max(first, 1), first + count
        cols = pl.ds(begin * LANES, (end - begin) * LANES)
        units = jnp.concatenate(
            [hid[s, :, :, cols].reshape(pair_rows, (end - begin) * LANES) for s in sets], axis=0
        )
        value = jnp.dot(units, down[down_rows(j), :], preferred_element_type=F32)
        for i, s in enumerate(sets):
            part = value[i * pair_rows:(i + 1) * pair_rows]
            if j == 0:
                part = part + adapter_part(s)
            if ("total", s) not in arrived:
                arrived.add(("total", s))
                total[s] = part
            else:
                total[s] += part

    def f_copy(r):
        return exp_copy(send_f.at[r], recv_f.at[r], f_send, f_recv, r)

    def finish(s, j):
        for r in ((0,) if s == NEAR else (1, 2)):
            at = pl.ds(pl.multiple_of(peers[r] % 2 * own_rows, own_rows), own_rows)
            send_f[r] = total[s, at, :].astype(BF16)
            f_copy(r).start()

    stages = {
        "product": product, "reduce": reduce, "activate": activate, "relay": relay,
        "project": project, "finish": finish,
    }
    for name, s, j in plan(spans):
        with jax.named_scope(f"{name}{s}{j}"):
            stages[name](s, j)

    with jax.named_scope("sends"):
        for copy in tok_copies + coef_copies:
            copy.wait_send()
        for s in range(2):
            for j in range(len(spans)):
                for make in (s1_copy, s2_copy, hp_copy, hx_copy, hr_copy):
                    make(s, j).wait_send()
    own = pl.ds(pl.multiple_of(me % 2 * own_rows, own_rows), own_rows)
    result = total[NEAR, own, :]
    for r in (1, 2, 0):
        with jax.named_scope(f"final{r}"):
            f_copy(r).wait_recv()
        result = result + recv_f[r].astype(F32)
    out_ref[...] = result.astype(out_ref.dtype)
    for r in range(3):
        f_copy(r).wait_send()


def fused(tokens, gate_up_weight, down_weight, adapter_in, adapter_out, expert_ids, route_weight):
    own_rows, feat = tokens.shape
    hidden = gate_up_weight.shape[2]
    tiles = hidden // LANES
    chunk_count = len(chunks_of(tiles + 1))
    wide = hidden + LANES
    top = expert_ids.shape[1]
    vmem = pltpu.VMEM
    dma = lambda *shape: pltpu.SemaphoreType.DMA(shape)
    in_place = pl.BlockSpec(memory_space=pltpu.HBM)
    pair = 2 * own_rows
    return pl.pallas_call(
        kernel,
        out_shape=jax.ShapeDtypeStruct((own_rows, feat), BF16),
        in_specs=[in_place] * 7,
        out_specs=pl.BlockSpec(memory_space=pltpu.VMEM),
        scratch_shapes=[
            vmem((tiles, 2 * feat, LANES), BF16),
            vmem((hidden, feat), BF16),
            vmem((4, own_rows, feat), BF16),
            vmem((LANES, feat), BF16),
            vmem((LANES, feat), BF16),
            vmem((top, own_rows), jnp.int32),
            vmem((top, own_rows), F32),
            vmem((3, 8, LANES), F32),
            vmem((4, 8, LANES), F32),
            vmem((4 * pair, 2 * feat), BF16),
            vmem((2, pair, wide), F32),
            vmem((2, pair, wide), BF16),
            vmem((2, pair, wide), BF16),
            vmem((2, pair, wide // 2), F32),
            vmem((2, pair, wide // 2), BF16),
            vmem((2, pair, wide // 2), BF16),
            vmem((2, 2, own_rows, wide), BF16),
            vmem((2, pair, feat), F32),
            vmem((3, own_rows, feat), BF16),
            vmem((3, own_rows, feat), BF16),
            dma(tiles), dma(chunk_count), dma(5),
            dma(3), dma(3), dma(3), dma(3),
            *[dma(2, chunk_count) for _ in range(10)],
            dma(3), dma(3),
        ],
        compiler_params=pltpu.CompilerParams(
            collective_id=0, has_side_effects=True, vmem_limit_bytes=60 * 2**20
        ),
    )(
        tokens, gate_up_weight, down_weight, jnp.swapaxes(adapter_in, 1, 2), adapter_out,
        expert_ids.T, route_weight.T,
    )


def plain(tokens, gate_up_weight, down_weight, adapter_in, adapter_out, expert_ids, route_weight):
    exp_count = lax.axis_size("exp")
    own_rows, feat_width = tokens.shape
    all_tokens = lax.all_gather(tokens, "exp", axis=0, tiled=True)
    hidden_width = gate_up_weight.shape[2]
    pair_weight = gate_up_weight.reshape(feat_width, 2 * hidden_width)
    pair_share = lax.psum_scatter(
        jnp.dot(all_tokens, pair_weight, preferred_element_type=jnp.float32).astype(jnp.bfloat16),
        "tp",
        scatter_dimension=0,
        tiled=True,
    ).astype(jnp.float32)
    hidden_share = (
        jax.nn.silu(pair_share[:, :hidden_width]) * pair_share[:, hidden_width:]
    ).astype(jnp.bfloat16)
    hidden = lax.all_gather(hidden_share, "tp", axis=0, tiled=True)
    base_out = lax.psum_scatter(
        jnp.dot(hidden, down_weight, preferred_element_type=jnp.float32).astype(jnp.bfloat16),
        "exp",
        scatter_dimension=0,
        tiled=True,
    ).astype(jnp.float32)
    top_count = expert_ids.shape[1]
    expert_count = adapter_in.shape[0] * exp_count
    flat_ids = expert_ids.reshape(own_rows * top_count)
    flat_weight = route_weight.reshape(own_rows * top_count)
    expert_hits = (flat_ids[:, None] == jnp.arange(expert_count, dtype=jnp.int32)[None, :]).astype(
        jnp.int32
    )
    capacity = max(2, 2 * top_count * own_rows // expert_count)
    slot_index = jnp.sum((jnp.cumsum(expert_hits, axis=0) - expert_hits) * expert_hits, axis=1)
    slot_target = flat_ids * capacity + slot_index
    slot_hits = (
        slot_target[:, None] == jnp.arange(expert_count * capacity, dtype=jnp.int32)[None, :]
    )
    combine_matrix = jnp.sum(
        (slot_hits.astype(jnp.float32) * flat_weight[:, None]).reshape(
            own_rows, top_count, expert_count * capacity
        ),
        axis=1,
    )
    dispatch_matrix = slot_hits.T.astype(jnp.bfloat16)
    repeated = jnp.repeat(tokens, top_count, axis=0)
    outgoing = jnp.dot(dispatch_matrix, repeated, preferred_element_type=jnp.float32).astype(
        jnp.bfloat16
    )
    outgoing = outgoing.reshape(expert_count, capacity, feat_width)
    rank_partial = jnp.einsum(
        "scd,dr->scr",
        lax.all_to_all(outgoing, "exp", split_axis=0, concat_axis=0, tiled=True),
        adapter_in[0],
        preferred_element_type=jnp.float32,
    )
    rank_mid = lax.psum(rank_partial, "tp").astype(jnp.bfloat16)
    expert_out = jnp.einsum(
        "scr,rd->scd", rank_mid, adapter_out[0], preferred_element_type=jnp.float32
    ).astype(jnp.bfloat16)
    returned = lax.all_to_all(expert_out, "exp", split_axis=0, concat_axis=0, tiled=True)
    adapter_sum = jnp.dot(
        combine_matrix,
        returned.reshape(expert_count * capacity, feat_width).astype(jnp.float32),
        precision=lax.Precision.HIGHEST,
        preferred_element_type=jnp.float32,
    )
    return (base_out + adapter_sum).astype(jnp.bfloat16)


def local(tokens, gate_up_weight, *rest):
    own_rows, feat = tokens.shape
    fits = (
        lax.axis_size("tp") == 4
        and lax.axis_size("exp") == 4
        and rest[1].shape[0] == 1
        and rest[1].shape[2] <= LANES
        and own_rows % 16 == 0
        and feat % LANES == 0
        and gate_up_weight.shape[2] % (2 * LANES) == LANES
    )
    return (fused if fits else plain)(tokens, gate_up_weight, *rest)


def solution(mesh):
    in_specs = (
        P(("grp", "exp"), "tp"),
        P("tp", None, "exp"),
        P("exp", "tp"),
        P("exp", "tp", None),
        P("exp", None, "tp"),
        P(("grp", "exp"), None),
        P(("grp", "exp"), None),
    )
    out_specs = P(("grp", "exp"), "tp")
    return jax.shard_map(local, mesh=mesh, in_specs=in_specs, out_specs=out_specs, check_vma=False)
```

```python
import functools
import jax
import jax.numpy as jnp
from jax import lax
from jax.experimental import pallas as pl
from jax.experimental.pallas import tpu as pltpu
from jax.sharding import PartitionSpec as P

LANES = 128
CHUNK_SHARES = (4, 8, 12, 10, 4)
MESH = pl.DeviceIdType.MESH
BF16, F32 = jnp.bfloat16, jnp.float32
NEAR, FAR = 0, 1

EARLY_STEPS = (
    ("PN0", "PN1", "RN0", "PN2", "RN1", "PB3", "RN2", "PB4", "PF2", "RN3", "RF3", "RN4", "RF4"),
    ("AN0", "PF1", "RF2", "AN1", "PF0", "RF1", "RF0", "AN2", "AN3", "AF3", "AN4", "AF4", "LN0"),
    ("AF2", "LN1", "AF1", "AF0", "DN01", "LN2", "LN3", "LF3", "LN4", "LF4", "DN2", "LF2", "LF1"),
    ("DN34", "ZN", "LF0", "DF234", "DF01", "ZF"),
)
LATE_STEPS = (
    ("PN0", "PN1", "PN2", "RN0", "RN1", "PF0", "PF1", "RN2", "RF0", "PF2", "RF1", "PB3", "RF2"),
    ("PB4", "RF3", "RF4", "AF0", "AF1", "RN3", "AF2", "AF3", "AF4", "RN4", "AN0", "AN1", "AN2"),
    ("LF0", "LF1", "LF2", "DF01", "LF3", "LF4", "AN3", "DF2", "AN4", "DF34", "ZF"),
    ("LN0", "LN1", "LN2", "DN01", "LN3", "DN2", "LN4", "DN34", "ZN"),
)


def chunks_of(columns):
    spans, first, passed = [], 0, 0
    for share in CHUNK_SHARES:
        passed += share
        end = 2 * (columns * passed // (2 * sum(CHUNK_SHARES)))
        spans.append((first, end - first))
        first = end
    return spans


def kernel(
    tok_ref, gu_ref, down_ref, ain_ref, aout_ref, ids_ref, weight_ref, out_ref,
    gu, down, tok_all, ain_pad, aout_pad, ids, weights, coef_own, coef_all, lhs,
    keep1, send1, recv1, keep2, send2, recv2, hid, total, send_f, recv_f,
    gu_sem, down_sem, in_sem, tok_send, tok_recv, coef_send, coef_recv,
    s1_recv, s2_recv, hx_recv, hq_recv, f_recv, s1_send, s2_send, hp_send, hx_send, hr_send,
    f_send, far_sem,
):
    me = lax.axis_index("exp")
    tp = lax.axis_index("tp")
    own_rows, feat = tok_ref.shape
    hidden = gu_ref.shape[2]
    rank = ain_ref.shape[1]
    tiles = hidden // LANES
    spans = chunks_of(tiles + 1)
    core, side = tp % 2, tp // 2
    partner = side * 2 + (1 - core)
    across = (1 - side) * 2 + core
    low = me - me % 2
    lows = (low, (low + 2) % 4)
    near = low + 1 - me % 2
    far = (me + 2) % 4
    peers = (near, far, (near + 2) % 4)

    late = me // 2

    barrier = pltpu.get_barrier_semaphore()
    for peer in (partner, across):
        pl.semaphore_signal(barrier, inc=1, device_id={"tp": peer}, device_id_type=MESH)
    pl.semaphore_signal(barrier, inc=1, device_id={"exp": near}, device_id_type=MESH)

    @pl.when(late == 0)
    def _():
        for peer in peers[1:]:
            pl.semaphore_signal(barrier, inc=1, device_id={"exp": peer}, device_id_type=MESH)

    in_copies = [
        pltpu.make_async_copy(tok_ref, tok_all.at[me], in_sem.at[0]),
        pltpu.make_async_copy(ids_ref, ids, in_sem.at[1]),
        pltpu.make_async_copy(weight_ref, weights, in_sem.at[2]),
        pltpu.make_async_copy(ain_ref.at[0], ain_pad.at[pl.ds(0, rank)], in_sem.at[3]),
        pltpu.make_async_copy(aout_ref.at[0], aout_pad.at[pl.ds(0, rank)], in_sem.at[4]),
    ]
    gu_flat = gu_ref.reshape(2 * feat, hidden)

    def gu_copy(t, j):
        cols = pl.ds(pl.multiple_of(t * LANES, LANES), LANES)
        return pltpu.make_async_copy(gu_flat.at[:, cols], gu.at[t], gu_sem.at[j])

    def gu_tiles(j):
        first, count = spans[j]
        return max(first - 1, 0), first + count - 1

    def gu_wait(j):
        begin, end = gu_tiles(j)
        ref = gu.at[pl.ds(begin, end - begin)]
        pltpu.make_async_copy(ref, ref, gu_sem.at[j]).wait()

    def down_rows(j):
        first, count = spans[j]
        begin, end = max(first - 1, 0), first + count - 1
        return pl.ds(begin * LANES, (end - begin) * LANES)

    def down_copy(j):
        rows = down_rows(j)
        return pltpu.make_async_copy(down_ref.at[rows], down.at[rows], down_sem.at[j])

    for copy in in_copies:
        copy.start()

    for j in range(len(spans)):

        def start_gu(t, carry):
            gu_copy(t, j).start()
            return carry

        lax.fori_loop(*gu_tiles(j), start_gu, 0)
    for j in range(len(spans)):
        down_copy(j).start()

    ain_pad[rank:, :] = jnp.zeros((LANES - rank, feat), BF16)
    aout_pad[rank:, :] = jnp.zeros((LANES - rank, feat), BF16)

    def exp_copy(src, dst, send, recv, r):
        return pltpu.make_async_remote_copy(
            src_ref=src, dst_ref=dst, send_sem=send.at[0], recv_sem=recv.at[r],
            device_id={"exp": peers[r]}, device_id_type=MESH,
        )

    tok_copies = [
        exp_copy(tok_all.at[me], tok_all.at[me], tok_send, tok_recv, r) for r in range(3)
    ]
    coef_copies = [
        exp_copy(
            coef_own.at[r, pl.ds(0, 1)], coef_all.at[me, pl.ds(0, 1)], coef_send, coef_recv, r
        )
        for r in range(3)
    ]
    pl.semaphore_wait(barrier, 3 + 2 * late)

    @pl.when(late == 1)
    def _():
        for peer in peers[1:]:
            pl.semaphore_signal(far_sem, inc=1, device_id={"exp": peer}, device_id_type=MESH)

    in_copies[0].wait()
    tok_copies[0].start()

    @pl.when(late == 1)
    def _():
        for copy in tok_copies[1:]:
            copy.start()

    in_copies[1].wait()
    in_copies[2].wait()

    def coef_line(expert):
        line = jnp.zeros((1, own_rows), F32)
        for k in range(ids.shape[0]):
            line = line + jnp.where(ids[k:k + 1, :] == expert, weights[k:k + 1, :], 0.0)
        return jnp.concatenate([line, jnp.zeros((1, LANES - own_rows), F32)], axis=1)

    for r in range(3):
        coef_own[r, 0:1, :] = coef_line(peers[r])
    coef_all[me, 0:1, :] = coef_line(me)
    coef_copies[0].start()

    @pl.when(late == 1)
    def _():
        for copy in coef_copies[1:]:
            copy.start()

    def span_cols(j):
        first, count = spans[j]
        return pl.ds(first * LANES, count * LANES)

    def half_cols(j, which):
        first, count = spans[j]
        width = count // 2 * LANES
        return pl.ds(pl.multiple_of(first * LANES + which * width, LANES), width)

    def pack_cols(j):
        first, count = spans[j]
        return pl.ds(first // 2 * LANES, count // 2 * LANES)

    def tp_copy(src, dst, send, recv, s, j, peer):
        return pltpu.make_async_remote_copy(
            src_ref=src, dst_ref=dst, send_sem=send.at[0], recv_sem=recv.at[s, j],
            device_id={"tp": peer}, device_id_type=MESH,
        )

    def s1_copy(s, j):
        cols = span_cols(j)
        return tp_copy(
            send1.at[s, :, cols], recv1.at[s, :, cols], s1_send, s1_recv, s, j, partner
        )

    def s2_copy(s, j):
        cols = pack_cols(j)
        return tp_copy(
            send2.at[s, :, cols], recv2.at[s, :, cols], s2_send, s2_recv, s, j, across
        )

    def hp_copy(s, j):
        ref = hid.at[s, core, :, half_cols(j, side)]
        return tp_copy(ref, ref, hp_send, hq_recv, s, j, partner)

    def hx_copy(s, j):
        ref = hid.at[s, core, :, half_cols(j, side)]
        return tp_copy(ref, ref, hx_send, hx_recv, s, j, across)

    def hr_copy(s, j):
        ref = hid.at[s, core, :, half_cols(j, 1 - side)]
        return tp_copy(ref, ref, hr_send, hq_recv, s, j, partner)

    def hq_wait(s, j):
        ref = hid.at[s, 1 - core, :, span_cols(j)]
        tp_copy(ref, ref, hp_send, hq_recv, s, j, partner).wait_recv()

    pair_rows = 2 * own_rows
    row = lax.broadcasted_iota(jnp.int32, (LANES, 4 * LANES), 0)
    col = lax.broadcasted_iota(jnp.int32, (LANES, 4 * LANES), 1)
    spread = jnp.where(col % (2 * LANES) == 2 * row + col // (2 * LANES), 1.0, 0.0).astype(BF16)

    def ordered(s):
        return jnp.concatenate([tok_all[lows[s] + core], tok_all[lows[s] + 1 - core]], axis=0)

    def prepare(s):
        for r in ((0,) if s == NEAR else (1, 2)):
            tok_copies[r].wait_recv()
        tokens = ordered(s)
        stacked = jnp.concatenate(
            [tokens[:, k * LANES:(k + 1) * LANES] for k in range(feat // LANES)], axis=0
        )
        wide = jnp.dot(stacked, spread, preferred_element_type=F32).astype(BF16)
        for k in range(feat // LANES):
            for p in range(2):
                for half in range(2):
                    to = 2 * s * pair_rows + (2 * p + half) * own_rows
                    lhs[to:to + own_rows, 2 * k * LANES:2 * (k + 1) * LANES] = wide[
                        k * pair_rows + p * own_rows:k * pair_rows + (p + 1) * own_rows,
                        2 * half * LANES:2 * (half + 1) * LANES,
                    ]
        if s == NEAR:
            in_copies[3].wait()
        value = lax.dot_general(
            tokens, ain_pad[...], (((1,), (1,)), ((), ())), preferred_element_type=F32
        )
        blank = jnp.zeros((own_rows, LANES), F32)
        store_pair(
            s, pl.ds(0, LANES),
            jnp.concatenate([value[:own_rows], blank, value[own_rows:], blank], axis=0),
        )

    def store_pair(s, cols, value):
        keep1[s, :, cols] = value[:pair_rows]
        send1[s, :, cols] = value[pair_rows:].astype(BF16)

    arrived = set()

    def product(sets, part):
        for s in sets:
            if s not in arrived:
                arrived.add(s)
                prepare(s)
        for j in part:
            if ("gu", j) not in arrived:
                arrived.add(("gu", j))
                gu_wait(j)
        rows = slice(0, 4 * pair_rows) if len(sets) == 2 else slice(
            2 * sets[0] * pair_rows, 2 * (sets[0] + 1) * pair_rows
        )
        for j in part:
            begin, end = gu_tiles(j)
            weight = jnp.concatenate([gu[t] for t in range(begin, end)], axis=1)
            value = jnp.dot(lhs[rows, :], weight, preferred_element_type=F32)
            cols = pl.ds((begin + 1) * LANES, (end - begin) * LANES)
            for s in sets:
                at = 2 * s * pair_rows if len(sets) == 2 else 0
                store_pair(s, cols, value[at:at + 2 * pair_rows])
                s1_copy(s, j).start()

    def reduce(s, j):
        s1_copy(s, j).wait_recv()
        cols = pack_cols(j)
        kept, sent = half_cols(j, side), half_cols(j, 1 - side)
        send2[s, :, cols] = (keep1[s, :, sent] + recv1[s, :, sent].astype(F32)).astype(BF16)
        s2_copy(s, j).start()
        keep2[s, :, cols] = keep1[s, :, kept] + recv1[s, :, kept].astype(F32)

    def activate(s, j):
        s2_copy(s, j).wait_recv()
        cols = pack_cols(j)
        pair = keep2[s, :, cols] + recv2[s, :, cols].astype(F32)
        value = jax.nn.silu(pair[:own_rows]) * pair[own_rows:]
        if j == 0:
            first = jnp.where(side == 0, pair[:own_rows, :LANES], value[:, :LANES])
            rest = [value[:, LANES:]] if value.shape[1] > LANES else []
            value = jnp.concatenate([first, *rest], axis=1)
        hid[s, core, :, half_cols(j, side)] = value.astype(BF16)
        hx_copy(s, j).start()
        hp_copy(s, j).start()

    def relay(s, j):
        hx_copy(s, j).wait_recv()
        hr_copy(s, j).start()

    diagonal = lax.broadcasted_iota(
        jnp.int32, (own_rows, own_rows), 0
    ) == lax.broadcasted_iota(jnp.int32, (own_rows, own_rows), 1)

    def adapter_part(s):
        if "out" not in arrived:
            arrived.add("out")
            in_copies[4].wait()
        for r in ((0,) if s == NEAR else (1, 2)):
            coef_copies[r].wait_recv()
        rank_mid = hid[s, :, :, pl.ds(0, LANES)].reshape(pair_rows, LANES)
        expert_out = jnp.dot(rank_mid, aout_pad[...], preferred_element_type=F32).astype(BF16)
        columns = []
        for c in range(2):
            line = coef_all[lows[s] + c, 0:1, :][:, :own_rows]
            columns.append(jnp.sum(jnp.where(diagonal, line, 0.0), axis=1, keepdims=True))
        return jnp.concatenate(columns, axis=0) * expert_out.astype(F32)

    def project(sets, part):
        for j in part:
            for s in sets:
                hq_wait(s, j)
            if ("down", j) not in arrived:
                arrived.add(("down", j))
                down_copy(j).wait()
        begin, end = max(spans[part[0]][0], 1), spans[part[-1]][0] + spans[part[-1]][1]
        cols = pl.ds(begin * LANES, (end - begin) * LANES)
        rows = pl.ds((begin - 1) * LANES, (end - begin) * LANES)
        units = jnp.concatenate(
            [hid[s, :, :, cols].reshape(pair_rows, (end - begin) * LANES) for s in sets], axis=0
        )
        value = jnp.dot(units, down[rows, :], preferred_element_type=F32)
        for i, s in enumerate(sets):
            share = value[i * pair_rows:(i + 1) * pair_rows]
            if part[0] == 0:
                share = share + adapter_part(s)
            if ("total", s) not in arrived:
                arrived.add(("total", s))
                total[s] = share
            else:
                total[s] += share

    def f_copy(r, peer):
        return pltpu.make_async_remote_copy(
            src_ref=send_f.at[r], dst_ref=recv_f.at[r],
            send_sem=f_send.at[0], recv_sem=f_recv.at[r],
            device_id={"exp": peer}, device_id_type=MESH,
        )

    def finish(s, late):
        if s == NEAR:
            targets = ((0, near),)
        elif late:
            targets = ((me - 1, 0), (4 - me, 1))
        else:
            targets = ((1, peers[1]), (2, peers[2]))
        for r, peer in targets:
            at = pl.ds(pl.multiple_of(peer % 2 * own_rows, own_rows), own_rows)
            send_f[r] = total[s, at, :].astype(BF16)
            f_copy(r, peer).start()

    single = {"R": reduce, "A": activate, "L": relay}
    sets_of = {"N": (NEAR,), "F": (FAR,), "B": (FAR, NEAR)}

    def run(which):
        arrived.clear()
        if not which:
            with jax.named_scope("open"):
                pl.semaphore_wait(far_sem, 2)
                for copy in tok_copies[1:] + coef_copies[1:]:
                    copy.start()
        for step in sum(LATE_STEPS if which else EARLY_STEPS, ()):
            kind, sets, part = step[0], sets_of[step[1]], tuple(int(c) for c in step[2:])
            with jax.named_scope(step):
                if kind == "Z":
                    finish(sets[0], which)
                elif kind == "D":
                    project(sets, part)
                elif kind == "P":
                    product(sets, part)
                else:
                    single[kind](sets[0], part[0])

    for which in range(2):
        pl.when(late == which)(functools.partial(run, which))

    with jax.named_scope("sends"):
        exp_copy(
            tok_all.at[pl.ds(0, 3)], tok_all.at[pl.ds(0, 3)], tok_send, tok_recv, 0
        ).wait_send()
        line = coef_own.at[:, pl.ds(0, 1)]
        exp_copy(line, line, coef_send, coef_recv, 0).wait_send()
        tp_copy(send1, recv1, s1_send, s1_recv, 0, 0, partner).wait_send()
        tp_copy(send2, recv2, s2_send, s2_recv, 0, 0, across).wait_send()
        part = hid.at[:, 0, :, pl.ds(0, (tiles + 1) // 2 * LANES)]
        for send in (hp_send, hx_send, hr_send):
            tp_copy(part, part, send, hx_recv, 0, 0, across).wait_send()
    own = pl.ds(pl.multiple_of(me % 2 * own_rows, own_rows), own_rows)
    result = total[NEAR, own, :]
    for r in (1, 2, 0):
        with jax.named_scope(f"final{r}"):
            f_copy(r, peers[r]).wait_recv()
        result = result + recv_f[r].astype(F32)
    out_ref[...] = result.astype(out_ref.dtype)
    exp_copy(send_f, recv_f, f_send, f_recv, 0).wait_send()


def fused(tokens, gate_up_weight, down_weight, adapter_in, adapter_out, expert_ids, route_weight):
    own_rows, feat = tokens.shape
    hidden = gate_up_weight.shape[2]
    tiles = hidden // LANES
    chunk_count = len(chunks_of(tiles + 1))
    wide = hidden + LANES
    top = expert_ids.shape[1]
    vmem = pltpu.VMEM
    dma = lambda *shape: pltpu.SemaphoreType.DMA(shape)
    in_place = pl.BlockSpec(memory_space=pltpu.HBM)
    pair = 2 * own_rows
    return pl.pallas_call(
        kernel,
        out_shape=pltpu.VMEM((own_rows, feat), BF16),
        in_specs=[in_place] * 7,
        out_specs=pl.BlockSpec(memory_space=pltpu.VMEM),
        scratch_shapes=[
            vmem((tiles, 2 * feat, LANES), BF16),
            vmem((hidden, feat), BF16),
            vmem((4, own_rows, feat), BF16),
            vmem((LANES, feat), BF16),
            vmem((LANES, feat), BF16),
            vmem((top, own_rows), jnp.int32),
            vmem((top, own_rows), F32),
            vmem((3, 8, LANES), F32),
            vmem((4, 8, LANES), F32),
            vmem((4 * pair, 2 * feat), BF16),
            vmem((2, pair, wide), F32),
            vmem((2, pair, wide), BF16),
            vmem((2, pair, wide), BF16),
            vmem((2, pair, wide // 2), F32),
            vmem((2, pair, wide // 2), BF16),
            vmem((2, pair, wide // 2), BF16),
            vmem((2, 2, own_rows, wide), BF16),
            vmem((2, pair, feat), F32),
            vmem((3, own_rows, feat), BF16),
            vmem((3, own_rows, feat), BF16),
            dma(chunk_count), dma(chunk_count), dma(5),
            dma(1), dma(3), dma(1), dma(3),
            *[dma(2, chunk_count) for _ in range(4)],
            dma(3), *[dma(1) for _ in range(6)],
            pltpu.SemaphoreType.REGULAR,
        ],
        compiler_params=pltpu.CompilerParams(
            collective_id=0, has_side_effects=True, vmem_limit_bytes=60 * 2**20
        ),
    )(
        tokens, gate_up_weight, down_weight, jnp.swapaxes(adapter_in, 1, 2), adapter_out,
        expert_ids.T, route_weight.T,
    )


def plain(tokens, gate_up_weight, down_weight, adapter_in, adapter_out, expert_ids, route_weight):
    exp_count = lax.axis_size("exp")
    own_rows, feat_width = tokens.shape
    all_tokens = lax.all_gather(tokens, "exp", axis=0, tiled=True)
    hidden_width = gate_up_weight.shape[2]
    pair_weight = gate_up_weight.reshape(feat_width, 2 * hidden_width)
    pair_share = lax.psum_scatter(
        jnp.dot(all_tokens, pair_weight, preferred_element_type=jnp.float32).astype(jnp.bfloat16),
        "tp",
        scatter_dimension=0,
        tiled=True,
    ).astype(jnp.float32)
    hidden_share = (
        jax.nn.silu(pair_share[:, :hidden_width]) * pair_share[:, hidden_width:]
    ).astype(jnp.bfloat16)
    hidden = lax.all_gather(hidden_share, "tp", axis=0, tiled=True)
    base_out = lax.psum_scatter(
        jnp.dot(hidden, down_weight, preferred_element_type=jnp.float32).astype(jnp.bfloat16),
        "exp",
        scatter_dimension=0,
        tiled=True,
    ).astype(jnp.float32)
    top_count = expert_ids.shape[1]
    expert_count = adapter_in.shape[0] * exp_count
    flat_ids = expert_ids.reshape(own_rows * top_count)
    flat_weight = route_weight.reshape(own_rows * top_count)
    expert_hits = (flat_ids[:, None] == jnp.arange(expert_count, dtype=jnp.int32)[None, :]).astype(
        jnp.int32
    )
    capacity = max(2, 2 * top_count * own_rows // expert_count)
    slot_index = jnp.sum((jnp.cumsum(expert_hits, axis=0) - expert_hits) * expert_hits, axis=1)
    slot_target = flat_ids * capacity + slot_index
    slot_hits = (
        slot_target[:, None] == jnp.arange(expert_count * capacity, dtype=jnp.int32)[None, :]
    )
    combine_matrix = jnp.sum(
        (slot_hits.astype(jnp.float32) * flat_weight[:, None]).reshape(
            own_rows, top_count, expert_count * capacity
        ),
        axis=1,
    )
    dispatch_matrix = slot_hits.T.astype(jnp.bfloat16)
    repeated = jnp.repeat(tokens, top_count, axis=0)
    outgoing = jnp.dot(dispatch_matrix, repeated, preferred_element_type=jnp.float32).astype(
        jnp.bfloat16
    )
    outgoing = outgoing.reshape(expert_count, capacity, feat_width)
    rank_partial = jnp.einsum(
        "scd,dr->scr",
        lax.all_to_all(outgoing, "exp", split_axis=0, concat_axis=0, tiled=True),
        adapter_in[0],
        preferred_element_type=jnp.float32,
    )
    rank_mid = lax.psum(rank_partial, "tp").astype(jnp.bfloat16)
    expert_out = jnp.einsum(
        "scr,rd->scd", rank_mid, adapter_out[0], preferred_element_type=jnp.float32
    ).astype(jnp.bfloat16)
    returned = lax.all_to_all(expert_out, "exp", split_axis=0, concat_axis=0, tiled=True)
    adapter_sum = jnp.dot(
        combine_matrix,
        returned.reshape(expert_count * capacity, feat_width).astype(jnp.float32),
        precision=lax.Precision.HIGHEST,
        preferred_element_type=jnp.float32,
    )
    return (base_out + adapter_sum).astype(jnp.bfloat16)


def local(tokens, gate_up_weight, *rest):
    own_rows, feat = tokens.shape
    fits = (
        lax.axis_size("tp") == 4
        and lax.axis_size("exp") == 4
        and rest[1].shape[0] == 1
        and rest[1].shape[2] <= LANES
        and own_rows % 16 == 0
        and feat % LANES == 0
        and gate_up_weight.shape[2] % (2 * LANES) == LANES
        and gate_up_weight.shape[2] >= 19 * LANES
    )
    return (fused if fits else plain)(tokens, gate_up_weight, *rest)


def solution(mesh):
    in_specs = (
        P(("grp", "exp"), "tp"),
        P("tp", None, "exp"),
        P("exp", "tp"),
        P("exp", "tp", None),
        P("exp", None, "tp"),
        P(("grp", "exp"), None),
        P(("grp", "exp"), None),
    )
    out_specs = P(("grp", "exp"), "tp")
    return jax.shard_map(local, mesh=mesh, in_specs=in_specs, out_specs=out_specs, check_vma=False)
```

```python
import functools
import jax
import jax.numpy as jnp
from jax import lax
from jax.experimental import pallas as pl
from jax.experimental.pallas import tpu as pltpu
from jax.sharding import PartitionSpec as P

LANES = 128
CHUNK_SHARES = (4, 8, 12, 10, 4)
PIECE_OF = (0, 0, 1, 2, 2)
MESH = pl.DeviceIdType.MESH
BF16, F32 = jnp.bfloat16, jnp.float32
NEAR, FAR = 0, 1

EARLY_STEPS = (
    ("PN0", "PN1", "RN0", "PN2", "RN1", "PB3", "RN2", "PB4", "PF2", "RN3", "RF3", "RN4", "RF4"),
    ("AN0", "PF1", "RF2", "AN1", "PF0", "RF1", "RF0", "AN2", "AN3", "AF3", "AN4", "AF4", "LN0"),
    ("AF2", "LN1", "AF1", "AF0", "DN01", "LN2", "LN3", "LF3", "LN4", "LF4", "DN2", "LF2", "LF1"),
    ("LF0", "DB34", "ZN", "DF2", "DF01", "ZF"),
)
LATE_STEPS = (
    ("PN0", "PN1", "PN2", "RN0", "RN1", "PF0", "PF1", "RN2", "RF0", "PF2", "RF1", "PB3", "RF2"),
    ("PB4", "RF3", "RF4", "AF0", "AF1", "RN3", "AF2", "RN4", "AF3", "AF4", "AN0", "AN1", "AN2"),
    ("LF0", "LF1", "AN3", "LF2", "DF01", "LF3", "LF4", "AN4", "DF2", "LN0", "LN1", "DF34", "ZF"),
    ("LN2", "DN01", "LN3", "LN4", "DN2", "DN34", "ZN"),
)


def chunks_of(columns):
    spans, first, passed = [], 0, 0
    for share in CHUNK_SHARES:
        passed += share
        end = 2 * (columns * passed // (2 * sum(CHUNK_SHARES)))
        spans.append((first, end - first))
        first = end
    return spans


def kernel(
    tok_ref, gu_ref, down_ref, ain_ref, aout_ref, ids_ref, weight_ref, out_ref,
    gu, down, tok_all, ain_pad, aout_pad, ids, weights, coef_own, coef_all, lhs,
    keep1, send1, recv1, keep2, send2, recv2, hid, total, send_f, recv_f,
    gu_sem, down_sem, in_sem, tok_send, tok_recv, coef_send, coef_recv,
    s1_recv, s2_recv, hx_recv, hq_recv, f_recv, s1_send, s2_send, hp_send, hx_send, hr_send,
    f_send, met_sem,
):
    me = lax.axis_index("exp")
    tp = lax.axis_index("tp")
    own_rows, feat = tok_ref.shape
    hidden = gu_ref.shape[2]
    rank = ain_ref.shape[1]
    tiles = hidden // LANES
    spans = chunks_of(tiles + 1)
    core, side = tp % 2, tp // 2
    partner = side * 2 + (1 - core)
    across = (1 - side) * 2 + core
    low = me - me % 2
    lows = (low, (low + 2) % 4)
    near = low + 1 - me % 2
    far = (me + 2) % 4
    peers = (near, far, (near + 2) % 4)

    late = me // 2
    barrier = pltpu.get_barrier_semaphore()

    def tell(condition, semaphore, axis, *targets):
        @pl.when(condition)
        def _():
            for peer in targets:
                pl.semaphore_signal(
                    semaphore, inc=1, device_id={axis: peer}, device_id_type=MESH
                )

    tell(late == 0, barrier, "exp", *peers[1:])
    tell(me >= 0, barrier, "exp", near)
    tell(side == 0, barrier, "tp", across)
    tell(core == 1, barrier, "tp", partner)

    in_copies = [
        pltpu.make_async_copy(tok_ref, tok_all.at[me], in_sem.at[0]),
        pltpu.make_async_copy(ids_ref, ids, in_sem.at[1]),
        pltpu.make_async_copy(weight_ref, weights, in_sem.at[2]),
        pltpu.make_async_copy(ain_ref.at[0], ain_pad.at[pl.ds(0, rank)], in_sem.at[3]),
        pltpu.make_async_copy(aout_ref.at[0], aout_pad.at[pl.ds(0, rank)], in_sem.at[4]),
    ]
    gu_flat = gu_ref.reshape(2 * feat, hidden)

    def gu_copy(t, j):
        cols = pl.ds(pl.multiple_of(t * LANES, LANES), LANES)
        return pltpu.make_async_copy(gu_flat.at[:, cols], gu.at[t], gu_sem.at[j])

    def gu_tiles(j):
        first, count = spans[j]
        return max(first - 1, 0), first + count - 1

    def gu_wait(j):
        begin, end = gu_tiles(j)
        ref = gu.at[pl.ds(begin, end - begin)]
        pltpu.make_async_copy(ref, ref, gu_sem.at[j]).wait()

    down_copy = pltpu.make_async_copy(down_ref, down, down_sem.at[0])

    for copy in in_copies:
        copy.start()

    for j in range(len(spans)):

        def start_gu(t, carry):
            gu_copy(t, j).start()
            return carry

        lax.fori_loop(*gu_tiles(j), start_gu, 0)
    down_copy.start()

    ain_pad[rank:, :] = jnp.zeros((LANES - rank, feat), BF16)
    aout_pad[rank:, :] = jnp.zeros((LANES - rank, feat), BF16)

    def exp_copy(src, dst, send, recv, r):
        return pltpu.make_async_remote_copy(
            src_ref=src, dst_ref=dst, send_sem=send.at[0], recv_sem=recv.at[r],
            device_id={"exp": peers[r]}, device_id_type=MESH,
        )

    tok_copies = [
        exp_copy(tok_all.at[me], tok_all.at[me], tok_send, tok_recv, r) for r in range(3)
    ]
    coef_copies = [
        exp_copy(
            coef_own.at[r, pl.ds(0, 1)], coef_all.at[me, pl.ds(0, 1)], coef_send, coef_recv, r
        )
        for r in range(3)
    ]
    pl.semaphore_wait(barrier, 2 * late + side + 2 - core)
    tell(late == 1, met_sem.at[0], "exp", *peers[1:])
    tell(side == 1, met_sem.at[1], "tp", across)
    tell(core == 0, met_sem.at[2], "tp", partner)
    in_copies[0].wait()

    def send_far(condition):
        @pl.when(condition)
        def _():
            for copy in tok_copies[1:]:
                copy.start()

    tok_copies[0].start()
    send_far(late == 1)

    in_copies[1].wait()
    in_copies[2].wait()

    def coef_line(expert):
        line = jnp.zeros((1, own_rows), F32)
        for k in range(ids.shape[0]):
            line = line + jnp.where(ids[k:k + 1, :] == expert, weights[k:k + 1, :], 0.0)
        return jnp.concatenate([line, jnp.zeros((1, LANES - own_rows), F32)], axis=1)

    for r in range(3):
        coef_own[r, 0:1, :] = coef_line(peers[r])
    coef_all[me, 0:1, :] = coef_line(me)
    coef_copies[0].start()

    @pl.when(late == 1)
    def _():
        for copy in coef_copies[1:]:
            copy.start()

    @pl.when(side == 0)
    def _():
        pl.semaphore_wait(met_sem.at[1], 1)

    @pl.when(core == 1)
    def _():
        pl.semaphore_wait(met_sem.at[2], 1)


    def span_cols(j):
        first, count = spans[j]
        return pl.ds(first * LANES, count * LANES)

    def half_cols(j, which):
        first, count = spans[j]
        width = count // 2 * LANES
        return pl.ds(pl.multiple_of(first * LANES + which * width, LANES), width)

    def pack_cols(j):
        first, count = spans[j]
        return pl.ds(first // 2 * LANES, count // 2 * LANES)

    def tp_copy(src, dst, send, recv, s, j, peer):
        return pltpu.make_async_remote_copy(
            src_ref=src, dst_ref=dst, send_sem=send.at[0], recv_sem=recv.at[s, j],
            device_id={"tp": peer}, device_id_type=MESH,
        )

    def s1_copy(s, j):
        cols = span_cols(j)
        return tp_copy(
            send1.at[s, :, cols], recv1.at[s, :, cols], s1_send, s1_recv, s, j, partner
        )

    def s2_copy(s, j):
        cols = pack_cols(j)
        return tp_copy(
            send2.at[s, :, cols], recv2.at[s, :, cols], s2_send, s2_recv, s, j, across
        )

    def hp_copy(s, j):
        ref = hid.at[s, core, :, half_cols(j, side)]
        return tp_copy(ref, ref, hp_send, hq_recv, s, PIECE_OF[j], partner)

    def hx_copy(s, j):
        ref = hid.at[s, core, :, half_cols(j, side)]
        return tp_copy(ref, ref, hx_send, hx_recv, s, j, across)

    def hr_copy(s, j):
        ref = hid.at[s, core, :, half_cols(j, 1 - side)]
        return tp_copy(ref, ref, hr_send, hq_recv, s, PIECE_OF[j], partner)

    def hq_wait(s, piece):
        members = [j for j in range(len(spans)) if PIECE_OF[j] == piece]
        first, (last, count) = spans[members[0]][0], spans[members[-1]]
        ref = hid.at[s, 1 - core, :, pl.ds(first * LANES, (last + count - first) * LANES)]
        tp_copy(ref, ref, hp_send, hq_recv, s, piece, partner).wait_recv()

    pair_rows = 2 * own_rows
    row = lax.broadcasted_iota(jnp.int32, (LANES, 4 * LANES), 0)
    col = lax.broadcasted_iota(jnp.int32, (LANES, 4 * LANES), 1)
    spread = jnp.where(col % (2 * LANES) == 2 * row + col // (2 * LANES), 1.0, 0.0).astype(BF16)

    def ordered(s):
        return jnp.concatenate([tok_all[lows[s] + core], tok_all[lows[s] + 1 - core]], axis=0)

    def prepare(s):
        for r in ((0,) if s == NEAR else (1, 2)):
            tok_copies[r].wait_recv()
        tokens = ordered(s)
        stacked = jnp.concatenate(
            [tokens[:, k * LANES:(k + 1) * LANES] for k in range(feat // LANES)], axis=0
        )
        wide = jnp.dot(stacked, spread, preferred_element_type=F32).astype(BF16)
        for k in range(feat // LANES):
            for p in range(2):
                for half in range(2):
                    to = 2 * s * pair_rows + (2 * p + half) * own_rows
                    lhs[to:to + own_rows, 2 * k * LANES:2 * (k + 1) * LANES] = wide[
                        k * pair_rows + p * own_rows:k * pair_rows + (p + 1) * own_rows,
                        2 * half * LANES:2 * (half + 1) * LANES,
                    ]
        if s == NEAR:
            in_copies[3].wait()
        value = lax.dot_general(
            tokens, ain_pad[...], (((1,), (1,)), ((), ())), preferred_element_type=F32
        )
        blank = jnp.zeros((own_rows, LANES), F32)
        store_pair(
            s, pl.ds(0, LANES),
            jnp.concatenate([value[:own_rows], blank, value[own_rows:], blank], axis=0),
        )

    def store_pair(s, cols, value):
        keep1[s, :, cols] = value[:pair_rows]
        send1[s, :, cols] = value[pair_rows:].astype(BF16)

    arrived = set()

    def product(sets, part):
        for s in sets:
            if s not in arrived:
                arrived.add(s)
                prepare(s)
        for j in part:
            if ("gu", j) not in arrived:
                arrived.add(("gu", j))
                gu_wait(j)
        rows = slice(0, 4 * pair_rows) if len(sets) == 2 else slice(
            2 * sets[0] * pair_rows, 2 * (sets[0] + 1) * pair_rows
        )
        for j in part:
            begin, end = gu_tiles(j)
            weight = jnp.concatenate([gu[t] for t in range(begin, end)], axis=1)
            value = jnp.dot(lhs[rows, :], weight, preferred_element_type=F32)
            cols = pl.ds((begin + 1) * LANES, (end - begin) * LANES)
            for s in sets:
                at = 2 * s * pair_rows if len(sets) == 2 else 0
                store_pair(s, cols, value[at:at + 2 * pair_rows])
                s1_copy(s, j).start()

    def reduce(s, j):
        s1_copy(s, j).wait_recv()
        cols = pack_cols(j)
        kept, sent = half_cols(j, side), half_cols(j, 1 - side)
        send2[s, :, cols] = (keep1[s, :, sent] + recv1[s, :, sent].astype(F32)).astype(BF16)
        s2_copy(s, j).start()
        keep2[s, :, cols] = keep1[s, :, kept] + recv1[s, :, kept].astype(F32)

    def activate(s, j):
        s2_copy(s, j).wait_recv()
        cols = pack_cols(j)
        pair = keep2[s, :, cols] + recv2[s, :, cols].astype(F32)
        value = jax.nn.silu(pair[:own_rows]) * pair[own_rows:]
        if j == 0:
            first = jnp.where(side == 0, pair[:own_rows, :LANES], value[:, :LANES])
            rest = [value[:, LANES:]] if value.shape[1] > LANES else []
            value = jnp.concatenate([first, *rest], axis=1)
        hid[s, core, :, half_cols(j, side)] = value.astype(BF16)
        hx_copy(s, j).start()
        hp_copy(s, j).start()

    def relay(s, j):
        hx_copy(s, j).wait_recv()
        hr_copy(s, j).start()

    diagonal = lax.broadcasted_iota(
        jnp.int32, (own_rows, own_rows), 0
    ) == lax.broadcasted_iota(jnp.int32, (own_rows, own_rows), 1)

    def adapter_part(s):
        if "out" not in arrived:
            arrived.add("out")
            in_copies[4].wait()
        for r in ((0,) if s == NEAR else (1, 2)):
            coef_copies[r].wait_recv()
        rank_mid = hid[s, :, :, pl.ds(0, LANES)].reshape(pair_rows, LANES)
        expert_out = jnp.dot(rank_mid, aout_pad[...], preferred_element_type=F32).astype(BF16)
        columns = []
        for c in range(2):
            line = coef_all[lows[s] + c, 0:1, :][:, :own_rows]
            columns.append(jnp.sum(jnp.where(diagonal, line, 0.0), axis=1, keepdims=True))
        return jnp.concatenate(columns, axis=0) * expert_out.astype(F32)

    def project(sets, part):
        for piece in sorted({PIECE_OF[j] for j in part}):
            for s in sets:
                hq_wait(s, piece)
        if "down" not in arrived:
            arrived.add("down")
            down_copy.wait()
        begin, end = max(spans[part[0]][0], 1), spans[part[-1]][0] + spans[part[-1]][1]
        cols = pl.ds(begin * LANES, (end - begin) * LANES)
        rows = pl.ds((begin - 1) * LANES, (end - begin) * LANES)
        units = jnp.concatenate(
            [hid[s, :, :, cols].reshape(pair_rows, (end - begin) * LANES) for s in sets], axis=0
        )
        value = jnp.dot(units, down[rows, :], preferred_element_type=F32)
        for i, s in enumerate(sets):
            share = value[i * pair_rows:(i + 1) * pair_rows]
            if part[0] == 0:
                share = share + adapter_part(s)
            if ("total", s) not in arrived:
                arrived.add(("total", s))
                total[s] = share
            else:
                total[s] += share

    def f_copy(r, peer):
        return pltpu.make_async_remote_copy(
            src_ref=send_f.at[r], dst_ref=recv_f.at[r],
            send_sem=f_send.at[0], recv_sem=f_recv.at[r],
            device_id={"exp": peer}, device_id_type=MESH,
        )

    def finish(s, late):
        if s == NEAR:
            targets = ((0, near),)
        elif late:
            targets = ((me - 1, 0), (4 - me, 1))
        else:
            targets = ((1, peers[1]), (2, peers[2]))
        for r, peer in targets:
            at = pl.ds(pl.multiple_of(peer % 2 * own_rows, own_rows), own_rows)
            send_f[r] = total[s, at, :].astype(BF16)
            f_copy(r, peer).start()

    single = {"R": reduce, "A": activate, "L": relay}
    sets_of = {"N": (NEAR,), "F": (FAR,), "B": (FAR, NEAR)}

    def run(which):
        arrived.clear()
        if not which:
            with jax.named_scope("open"):
                pl.semaphore_wait(met_sem.at[0], 2)
                for copy in tok_copies[1:] + coef_copies[1:]:
                    copy.start()
        for step in sum(LATE_STEPS if which else EARLY_STEPS, ()):
            kind, sets, part = step[0], sets_of[step[1]], tuple(int(c) for c in step[2:])
            with jax.named_scope(step):
                if kind == "Z":
                    finish(sets[0], which)
                elif kind == "D":
                    project(sets, part)
                elif kind == "P":
                    product(sets, part)
                else:
                    single[kind](sets[0], part[0])

    for which in range(2):
        pl.when(late == which)(functools.partial(run, which))

    with jax.named_scope("sends"):
        exp_copy(
            tok_all.at[pl.ds(0, 3)], tok_all.at[pl.ds(0, 3)], tok_send, tok_recv, 0
        ).wait_send()
        line = coef_own.at[:, pl.ds(0, 1)]
        exp_copy(line, line, coef_send, coef_recv, 0).wait_send()
        tp_copy(send1, recv1, s1_send, s1_recv, 0, 0, partner).wait_send()
        tp_copy(send2, recv2, s2_send, s2_recv, 0, 0, across).wait_send()
        part = hid.at[:, 0, :, pl.ds(0, (tiles + 1) // 2 * LANES)]
        for send in (hp_send, hx_send, hr_send):
            tp_copy(part, part, send, hx_recv, 0, 0, across).wait_send()
    own = pl.ds(pl.multiple_of(me % 2 * own_rows, own_rows), own_rows)
    result = total[NEAR, own, :]
    for r in (1, 2, 0):
        with jax.named_scope(f"final{r}"):
            f_copy(r, peers[r]).wait_recv()
        result = result + recv_f[r].astype(F32)
    out_ref[...] = result.astype(out_ref.dtype)
    exp_copy(send_f, recv_f, f_send, f_recv, 0).wait_send()


def fused(tokens, gate_up_weight, down_weight, adapter_in, adapter_out, expert_ids, route_weight):
    own_rows, feat = tokens.shape
    hidden = gate_up_weight.shape[2]
    tiles = hidden // LANES
    chunk_count = len(chunks_of(tiles + 1))
    wide = hidden + LANES
    top = expert_ids.shape[1]
    vmem = pltpu.VMEM
    dma = lambda *shape: pltpu.SemaphoreType.DMA(shape)
    in_place = pl.BlockSpec(memory_space=pltpu.HBM)
    pair = 2 * own_rows
    return pl.pallas_call(
        kernel,
        out_shape=pltpu.VMEM((own_rows, feat), BF16),
        in_specs=[in_place] * 7,
        out_specs=pl.BlockSpec(memory_space=pltpu.VMEM),
        scratch_shapes=[
            vmem((tiles, 2 * feat, LANES), BF16),
            vmem((hidden, feat), BF16),
            vmem((4, own_rows, feat), BF16),
            vmem((LANES, feat), BF16),
            vmem((LANES, feat), BF16),
            vmem((top, own_rows), jnp.int32),
            vmem((top, own_rows), F32),
            vmem((3, 8, LANES), F32),
            vmem((4, 8, LANES), F32),
            vmem((4 * pair, 2 * feat), BF16),
            vmem((2, pair, wide), F32),
            vmem((2, pair, wide), BF16),
            vmem((2, pair, wide), BF16),
            vmem((2, pair, wide // 2), F32),
            vmem((2, pair, wide // 2), BF16),
            vmem((2, pair, wide // 2), BF16),
            vmem((2, 2, own_rows, wide), BF16),
            vmem((2, pair, feat), F32),
            vmem((3, own_rows, feat), BF16),
            vmem((3, own_rows, feat), BF16),
            dma(chunk_count), dma(1), dma(5),
            dma(1), dma(3), dma(1), dma(3),
            *[dma(2, chunk_count) for _ in range(3)], dma(2, PIECE_OF[-1] + 1),
            dma(3), *[dma(1) for _ in range(6)],
            pltpu.SemaphoreType.REGULAR((3,)),
        ],
        compiler_params=pltpu.CompilerParams(
            collective_id=0, has_side_effects=True, vmem_limit_bytes=60 * 2**20
        ),
    )(
        tokens, gate_up_weight, down_weight, jnp.swapaxes(adapter_in, 1, 2), adapter_out,
        expert_ids.T, route_weight.T,
    )


def plain(tokens, gate_up_weight, down_weight, adapter_in, adapter_out, expert_ids, route_weight):
    exp_count = lax.axis_size("exp")
    own_rows, feat_width = tokens.shape
    all_tokens = lax.all_gather(tokens, "exp", axis=0, tiled=True)
    hidden_width = gate_up_weight.shape[2]
    pair_weight = gate_up_weight.reshape(feat_width, 2 * hidden_width)
    pair_share = lax.psum_scatter(
        jnp.dot(all_tokens, pair_weight, preferred_element_type=jnp.float32).astype(jnp.bfloat16),
        "tp",
        scatter_dimension=0,
        tiled=True,
    ).astype(jnp.float32)
    hidden_share = (
        jax.nn.silu(pair_share[:, :hidden_width]) * pair_share[:, hidden_width:]
    ).astype(jnp.bfloat16)
    hidden = lax.all_gather(hidden_share, "tp", axis=0, tiled=True)
    base_out = lax.psum_scatter(
        jnp.dot(hidden, down_weight, preferred_element_type=jnp.float32).astype(jnp.bfloat16),
        "exp",
        scatter_dimension=0,
        tiled=True,
    ).astype(jnp.float32)
    top_count = expert_ids.shape[1]
    expert_count = adapter_in.shape[0] * exp_count
    flat_ids = expert_ids.reshape(own_rows * top_count)
    flat_weight = route_weight.reshape(own_rows * top_count)
    expert_hits = (flat_ids[:, None] == jnp.arange(expert_count, dtype=jnp.int32)[None, :]).astype(
        jnp.int32
    )
    capacity = max(2, 2 * top_count * own_rows // expert_count)
    slot_index = jnp.sum((jnp.cumsum(expert_hits, axis=0) - expert_hits) * expert_hits, axis=1)
    slot_target = flat_ids * capacity + slot_index
    slot_hits = (
        slot_target[:, None] == jnp.arange(expert_count * capacity, dtype=jnp.int32)[None, :]
    )
    combine_matrix = jnp.sum(
        (slot_hits.astype(jnp.float32) * flat_weight[:, None]).reshape(
            own_rows, top_count, expert_count * capacity
        ),
        axis=1,
    )
    dispatch_matrix = slot_hits.T.astype(jnp.bfloat16)
    repeated = jnp.repeat(tokens, top_count, axis=0)
    outgoing = jnp.dot(dispatch_matrix, repeated, preferred_element_type=jnp.float32).astype(
        jnp.bfloat16
    )
    outgoing = outgoing.reshape(expert_count, capacity, feat_width)
    rank_partial = jnp.einsum(
        "scd,dr->scr",
        lax.all_to_all(outgoing, "exp", split_axis=0, concat_axis=0, tiled=True),
        adapter_in[0],
        preferred_element_type=jnp.float32,
    )
    rank_mid = lax.psum(rank_partial, "tp").astype(jnp.bfloat16)
    expert_out = jnp.einsum(
        "scr,rd->scd", rank_mid, adapter_out[0], preferred_element_type=jnp.float32
    ).astype(jnp.bfloat16)
    returned = lax.all_to_all(expert_out, "exp", split_axis=0, concat_axis=0, tiled=True)
    adapter_sum = jnp.dot(
        combine_matrix,
        returned.reshape(expert_count * capacity, feat_width).astype(jnp.float32),
        precision=lax.Precision.HIGHEST,
        preferred_element_type=jnp.float32,
    )
    return (base_out + adapter_sum).astype(jnp.bfloat16)


def local(tokens, gate_up_weight, *rest):
    own_rows, feat = tokens.shape
    fits = (
        lax.axis_size("tp") == 4
        and lax.axis_size("exp") == 4
        and rest[1].shape[0] == 1
        and rest[1].shape[2] <= LANES
        and own_rows % 16 == 0
        and feat % LANES == 0
        and gate_up_weight.shape[2] % (2 * LANES) == LANES
        and gate_up_weight.shape[2] >= 19 * LANES
    )
    return (fused if fits else plain)(tokens, gate_up_weight, *rest)


def solution(mesh):
    in_specs = (
        P(("grp", "exp"), "tp"),
        P("tp", None, "exp"),
        P("exp", "tp"),
        P("exp", "tp", None),
        P("exp", None, "tp"),
        P(("grp", "exp"), None),
        P(("grp", "exp"), None),
    )
    out_specs = P(("grp", "exp"), "tp")
    return jax.shard_map(local, mesh=mesh, in_specs=in_specs, out_specs=out_specs, check_vma=False)
```

```python
import functools
import jax
import jax.numpy as jnp
from jax import lax
from jax.experimental import pallas as pl
from jax.experimental.pallas import tpu as pltpu
from jax.sharding import PartitionSpec as P

LANES = 128
CHUNK_SHARES = (4, 8, 12, 10, 4)
PIECE_OF = (0, 0, 1, 2, 2)
MESH = pl.DeviceIdType.MESH
BF16, F32 = jnp.bfloat16, jnp.float32
NEAR, FAR = 0, 1

EARLY_STEPS = (
    ("PN0", "PN1", "RN0", "PN2", "RN1", "PB3", "RN2", "PB4", "PF2", "RN3", "RF3", "RN4", "RF4"),
    ("AN0", "PF1", "RF2", "AN1", "PF0", "RF1", "RF0", "AN2", "AN3", "AF3", "AN4", "AF4", "LN0"),
    ("AF2", "LN1", "AF1", "AF0", "DN01", "LN2", "LN3", "LF3", "LN4", "LF4", "DN2", "LF2", "LF1"),
    ("LF0", "DB34", "ZN", "DF2", "DF01", "ZF"),
)
LATE_STEPS = (
    ("PN0", "PN1", "PN2", "RN0", "RN1", "PF2", "RN2", "PF1", "PF0", "RF2", "PB3", "RF1", "RF0"),
    ("PB4", "RF3", "RF4", "RN3", "AF2", "AF1", "AF0", "RN4", "AF3", "AF4", "AN0", "AN1", "AN2"),
    ("LF2", "AN3", "LF1", "LF0", "DF2", "LF3", "LF4", "AN4", "DF01", "LN0", "LN1", "DF34", "ZF"),
    ("LN2", "DN01", "LN3", "LN4", "DN2", "DN34", "ZN"),
)


def chunks_of(columns):
    spans, first, passed = [], 0, 0
    for share in CHUNK_SHARES:
        passed += share
        end = 2 * (columns * passed // (2 * sum(CHUNK_SHARES)))
        spans.append((first, end - first))
        first = end
    return spans


def kernel(
    tok_ref, gu_ref, down_ref, ain_ref, aout_ref, ids_ref, weight_ref, out_ref,
    gu, down, tok_all, ain_pad, aout_pad, ids, weights, coef_own, coef_all, lhs,
    keep1, send1, recv1, keep2, send2, recv2, hid, total, send_f, recv_f,
    gu_sem, down_sem, in_sem, tok_send, tok_recv, coef_send, coef_recv,
    s1_recv, s2_recv, hx_recv, hq_recv, f_recv, s1_send, s2_send, hp_send, hx_send, hr_send,
    f_send, met_sem,
):
    me = lax.axis_index("exp")
    tp = lax.axis_index("tp")
    own_rows, feat = tok_ref.shape
    hidden = gu_ref.shape[2]
    rank = ain_ref.shape[1]
    tiles = hidden // LANES
    spans = chunks_of(tiles + 1)
    core, side = tp % 2, tp // 2
    partner = side * 2 + (1 - core)
    across = (1 - side) * 2 + core
    low = me - me % 2
    lows = (low, (low + 2) % 4)
    near = low + 1 - me % 2
    far = (me + 2) % 4
    peers = (near, far, (near + 2) % 4)

    late = me // 2
    barrier = pltpu.get_barrier_semaphore()

    def tell(condition, semaphore, axis, *targets):
        @pl.when(condition)
        def _():
            for peer in targets:
                pl.semaphore_signal(
                    semaphore, inc=1, device_id={axis: peer}, device_id_type=MESH
                )

    tell(late == 0, barrier, "exp", *peers[1:])
    tell(me >= 0, barrier, "exp", near)
    tell(side == 0, barrier, "tp", across)
    tell(core == 1, barrier, "tp", partner)

    in_copies = [
        pltpu.make_async_copy(tok_ref, tok_all.at[me], in_sem.at[0]),
        pltpu.make_async_copy(ids_ref, ids, in_sem.at[1]),
        pltpu.make_async_copy(weight_ref, weights, in_sem.at[2]),
        pltpu.make_async_copy(ain_ref.at[0], ain_pad.at[pl.ds(0, rank)], in_sem.at[3]),
        pltpu.make_async_copy(aout_ref.at[0], aout_pad.at[pl.ds(0, rank)], in_sem.at[4]),
    ]
    gu_flat = gu_ref.reshape(2 * feat, hidden)

    def gu_copy(t, j):
        cols = pl.ds(pl.multiple_of(t * LANES, LANES), LANES)
        return pltpu.make_async_copy(gu_flat.at[:, cols], gu.at[t], gu_sem.at[j])

    def gu_tiles(j):
        first, count = spans[j]
        return max(first - 1, 0), first + count - 1

    def gu_wait(j):
        begin, end = gu_tiles(j)
        ref = gu.at[pl.ds(begin, end - begin)]
        pltpu.make_async_copy(ref, ref, gu_sem.at[j]).wait()

    down_copy = pltpu.make_async_copy(down_ref, down, down_sem.at[0])

    for copy in in_copies:
        copy.start()

    for j in range(len(spans)):

        def start_gu(t, carry):
            gu_copy(t, j).start()
            return carry

        lax.fori_loop(*gu_tiles(j), start_gu, 0)
    down_copy.start()

    ain_pad[rank:, :] = jnp.zeros((LANES - rank, feat), BF16)
    aout_pad[rank:, :] = jnp.zeros((LANES - rank, feat), BF16)

    def exp_copy(src, dst, send, recv, r):
        return pltpu.make_async_remote_copy(
            src_ref=src, dst_ref=dst, send_sem=send.at[0], recv_sem=recv.at[r],
            device_id={"exp": peers[r]}, device_id_type=MESH,
        )

    tok_copies = [
        exp_copy(tok_all.at[me], tok_all.at[me], tok_send, tok_recv, r) for r in range(3)
    ]
    coef_copies = [
        exp_copy(
            coef_own.at[r, pl.ds(0, 1)], coef_all.at[me, pl.ds(0, 1)], coef_send, coef_recv, r
        )
        for r in range(3)
    ]
    pl.semaphore_wait(barrier, 2 * late + side + 2 - core)
    tell(late == 1, met_sem.at[0], "exp", *peers[1:])
    tell(side == 1, met_sem.at[1], "tp", across)
    tell(core == 0, met_sem.at[2], "tp", partner)
    in_copies[0].wait()

    def send_far(condition):
        @pl.when(condition)
        def _():
            for copy in tok_copies[1:]:
                copy.start()

    tok_copies[0].start()
    send_far(late == 1)

    in_copies[1].wait()
    in_copies[2].wait()

    def coef_line(expert):
        line = jnp.zeros((1, own_rows), F32)
        for k in range(ids.shape[0]):
            line = line + jnp.where(ids[k:k + 1, :] == expert, weights[k:k + 1, :], 0.0)
        return jnp.concatenate([line, jnp.zeros((1, LANES - own_rows), F32)], axis=1)

    for r in range(3):
        coef_own[r, 0:1, :] = coef_line(peers[r])
    coef_all[me, 0:1, :] = coef_line(me)
    coef_copies[0].start()

    @pl.when(late == 1)
    def _():
        for copy in coef_copies[1:]:
            copy.start()

    @pl.when(side == 0)
    def _():
        pl.semaphore_wait(met_sem.at[1], 1)

    @pl.when(core == 1)
    def _():
        pl.semaphore_wait(met_sem.at[2], 1)


    def span_cols(j):
        first, count = spans[j]
        return pl.ds(first * LANES, count * LANES)

    def half_cols(j, which):
        first, count = spans[j]
        width = count // 2 * LANES
        return pl.ds(pl.multiple_of(first * LANES + which * width, LANES), width)

    def pack_cols(j):
        first, count = spans[j]
        return pl.ds(first // 2 * LANES, count // 2 * LANES)

    def tp_copy(src, dst, send, recv, s, j, peer):
        return pltpu.make_async_remote_copy(
            src_ref=src, dst_ref=dst, send_sem=send.at[0], recv_sem=recv.at[s, j],
            device_id={"tp": peer}, device_id_type=MESH,
        )

    def s1_copy(s, j):
        cols = span_cols(j)
        return tp_copy(
            send1.at[s, :, cols], recv1.at[s, :, cols], s1_send, s1_recv, s, j, partner
        )

    def s2_copy(s, j):
        cols = pack_cols(j)
        return tp_copy(
            send2.at[s, :, cols], recv2.at[s, :, cols], s2_send, s2_recv, s, j, across
        )

    def hp_copy(s, j):
        ref = hid.at[s, core, :, half_cols(j, side)]
        return tp_copy(ref, ref, hp_send, hq_recv, s, PIECE_OF[j], partner)

    def hx_copy(s, j):
        ref = hid.at[s, core, :, half_cols(j, side)]
        return tp_copy(ref, ref, hx_send, hx_recv, s, j, across)

    def hr_copy(s, j):
        ref = hid.at[s, core, :, half_cols(j, 1 - side)]
        return tp_copy(ref, ref, hr_send, hq_recv, s, PIECE_OF[j], partner)

    def hq_wait(s, piece):
        members = [j for j in range(len(spans)) if PIECE_OF[j] == piece]
        first, (last, count) = spans[members[0]][0], spans[members[-1]]
        ref = hid.at[s, 1 - core, :, pl.ds(first * LANES, (last + count - first) * LANES)]
        tp_copy(ref, ref, hp_send, hq_recv, s, piece, partner).wait_recv()

    pair_rows = 2 * own_rows
    row = lax.broadcasted_iota(jnp.int32, (LANES, 4 * LANES), 0)
    col = lax.broadcasted_iota(jnp.int32, (LANES, 4 * LANES), 1)
    spread = jnp.where(col % (2 * LANES) == 2 * row + col // (2 * LANES), 1.0, 0.0).astype(BF16)

    def ordered(s):
        return jnp.concatenate([tok_all[lows[s] + core], tok_all[lows[s] + 1 - core]], axis=0)

    def prepare(s):
        for r in ((0,) if s == NEAR else (1, 2)):
            tok_copies[r].wait_recv()
        tokens = ordered(s)
        stacked = jnp.concatenate(
            [tokens[:, k * LANES:(k + 1) * LANES] for k in range(feat // LANES)], axis=0
        )
        wide = jnp.dot(stacked, spread, preferred_element_type=F32).astype(BF16)
        for k in range(feat // LANES):
            for p in range(2):
                for half in range(2):
                    to = 2 * s * pair_rows + (2 * p + half) * own_rows
                    lhs[to:to + own_rows, 2 * k * LANES:2 * (k + 1) * LANES] = wide[
                        k * pair_rows + p * own_rows:k * pair_rows + (p + 1) * own_rows,
                        2 * half * LANES:2 * (half + 1) * LANES,
                    ]
        if s == NEAR:
            in_copies[3].wait()
        value = lax.dot_general(
            tokens, ain_pad[...], (((1,), (1,)), ((), ())), preferred_element_type=F32
        )
        blank = jnp.zeros((own_rows, LANES), F32)
        store_pair(
            s, pl.ds(0, LANES),
            jnp.concatenate([value[:own_rows], blank, value[own_rows:], blank], axis=0),
        )

    def store_pair(s, cols, value):
        keep1[s, :, cols] = value[:pair_rows]
        send1[s, :, cols] = value[pair_rows:].astype(BF16)

    arrived = set()

    def product(sets, part):
        for s in sets:
            if s not in arrived:
                arrived.add(s)
                prepare(s)
        for j in part:
            if ("gu", j) not in arrived:
                arrived.add(("gu", j))
                gu_wait(j)
        rows = slice(0, 4 * pair_rows) if len(sets) == 2 else slice(
            2 * sets[0] * pair_rows, 2 * (sets[0] + 1) * pair_rows
        )
        for j in part:
            begin, end = gu_tiles(j)
            weight = jnp.concatenate([gu[t] for t in range(begin, end)], axis=1)
            value = jnp.dot(lhs[rows, :], weight, preferred_element_type=F32)
            cols = pl.ds((begin + 1) * LANES, (end - begin) * LANES)
            for s in sets:
                at = 2 * s * pair_rows if len(sets) == 2 else 0
                store_pair(s, cols, value[at:at + 2 * pair_rows])
                s1_copy(s, j).start()

    def reduce(s, j):
        s1_copy(s, j).wait_recv()
        cols = pack_cols(j)
        kept, sent = half_cols(j, side), half_cols(j, 1 - side)
        send2[s, :, cols] = (keep1[s, :, sent] + recv1[s, :, sent].astype(F32)).astype(BF16)
        s2_copy(s, j).start()
        keep2[s, :, cols] = keep1[s, :, kept] + recv1[s, :, kept].astype(F32)

    def activate(s, j):
        s2_copy(s, j).wait_recv()
        cols = pack_cols(j)
        pair = keep2[s, :, cols] + recv2[s, :, cols].astype(F32)
        value = jax.nn.silu(pair[:own_rows]) * pair[own_rows:]
        if j == 0:
            first = jnp.where(side == 0, pair[:own_rows, :LANES], value[:, :LANES])
            rest = [value[:, LANES:]] if value.shape[1] > LANES else []
            value = jnp.concatenate([first, *rest], axis=1)
        hid[s, core, :, half_cols(j, side)] = value.astype(BF16)
        hx_copy(s, j).start()
        hp_copy(s, j).start()

    def relay(s, j):
        hx_copy(s, j).wait_recv()
        hr_copy(s, j).start()

    diagonal = lax.broadcasted_iota(
        jnp.int32, (own_rows, own_rows), 0
    ) == lax.broadcasted_iota(jnp.int32, (own_rows, own_rows), 1)

    def adapter_part(s):
        if "out" not in arrived:
            arrived.add("out")
            in_copies[4].wait()
        for r in ((0,) if s == NEAR else (1, 2)):
            coef_copies[r].wait_recv()
        rank_mid = hid[s, :, :, pl.ds(0, LANES)].reshape(pair_rows, LANES)
        expert_out = jnp.dot(rank_mid, aout_pad[...], preferred_element_type=F32).astype(BF16)
        columns = []
        for c in range(2):
            line = coef_all[lows[s] + c, 0:1, :][:, :own_rows]
            columns.append(jnp.sum(jnp.where(diagonal, line, 0.0), axis=1, keepdims=True))
        return jnp.concatenate(columns, axis=0) * expert_out.astype(F32)

    def project(sets, part):
        for piece in sorted({PIECE_OF[j] for j in part}):
            for s in sets:
                hq_wait(s, piece)
        if "down" not in arrived:
            arrived.add("down")
            down_copy.wait()
        begin, end = max(spans[part[0]][0], 1), spans[part[-1]][0] + spans[part[-1]][1]
        cols = pl.ds(begin * LANES, (end - begin) * LANES)
        rows = pl.ds((begin - 1) * LANES, (end - begin) * LANES)
        units = jnp.concatenate(
            [hid[s, :, :, cols].reshape(pair_rows, (end - begin) * LANES) for s in sets], axis=0
        )
        value = jnp.dot(units, down[rows, :], preferred_element_type=F32)
        for i, s in enumerate(sets):
            share = value[i * pair_rows:(i + 1) * pair_rows]
            if part[0] == 0:
                share = share + adapter_part(s)
            if ("total", s) not in arrived:
                arrived.add(("total", s))
                total[s] = share
            else:
                total[s] += share

    def f_copy(r, peer):
        return pltpu.make_async_remote_copy(
            src_ref=send_f.at[r], dst_ref=recv_f.at[r],
            send_sem=f_send.at[0], recv_sem=f_recv.at[r],
            device_id={"exp": peer}, device_id_type=MESH,
        )

    def finish(s, late):
        if s == NEAR:
            targets = ((0, near),)
        elif late:
            targets = ((me - 1, 0), (4 - me, 1))
        else:
            targets = ((1, peers[1]), (2, peers[2]))
        for r, peer in targets:
            at = pl.ds(pl.multiple_of(peer % 2 * own_rows, own_rows), own_rows)
            send_f[r] = total[s, at, :].astype(BF16)
            f_copy(r, peer).start()

    single = {"R": reduce, "A": activate, "L": relay}
    sets_of = {"N": (NEAR,), "F": (FAR,), "B": (FAR, NEAR)}

    def run(which):
        arrived.clear()
        if not which:
            with jax.named_scope("open"):
                pl.semaphore_wait(met_sem.at[0], 2)
                for copy in tok_copies[1:] + coef_copies[1:]:
                    copy.start()
        for step in sum(LATE_STEPS if which else EARLY_STEPS, ()):
            kind, sets, part = step[0], sets_of[step[1]], tuple(int(c) for c in step[2:])
            with jax.named_scope(step):
                if kind == "Z":
                    finish(sets[0], which)
                elif kind == "D":
                    project(sets, part)
                elif kind == "P":
                    product(sets, part)
                else:
                    single[kind](sets[0], part[0])

    for which in range(2):
        pl.when(late == which)(functools.partial(run, which))

    with jax.named_scope("sends"):
        exp_copy(
            tok_all.at[pl.ds(0, 3)], tok_all.at[pl.ds(0, 3)], tok_send, tok_recv, 0
        ).wait_send()
        line = coef_own.at[:, pl.ds(0, 1)]
        exp_copy(line, line, coef_send, coef_recv, 0).wait_send()
        tp_copy(send1, recv1, s1_send, s1_recv, 0, 0, partner).wait_send()
        tp_copy(send2, recv2, s2_send, s2_recv, 0, 0, across).wait_send()
        part = hid.at[:, 0, :, pl.ds(0, (tiles + 1) // 2 * LANES)]
        for send in (hp_send, hx_send, hr_send):
            tp_copy(part, part, send, hx_recv, 0, 0, across).wait_send()
    own = pl.ds(pl.multiple_of(me % 2 * own_rows, own_rows), own_rows)
    result = total[NEAR, own, :]
    for r in (1, 2, 0):
        with jax.named_scope(f"final{r}"):
            f_copy(r, peers[r]).wait_recv()
        result = result + recv_f[r].astype(F32)
    out_ref[...] = result.astype(out_ref.dtype)
    exp_copy(send_f, recv_f, f_send, f_recv, 0).wait_send()


def fused(tokens, gate_up_weight, down_weight, adapter_in, adapter_out, expert_ids, route_weight):
    own_rows, feat = tokens.shape
    hidden = gate_up_weight.shape[2]
    tiles = hidden // LANES
    chunk_count = len(chunks_of(tiles + 1))
    wide = hidden + LANES
    top = expert_ids.shape[1]
    vmem = pltpu.VMEM
    dma = lambda *shape: pltpu.SemaphoreType.DMA(shape)
    in_place = pl.BlockSpec(memory_space=pltpu.HBM)
    pair = 2 * own_rows
    return pl.pallas_call(
        kernel,
        out_shape=pltpu.VMEM((own_rows, feat), BF16),
        in_specs=[in_place] * 7,
        out_specs=pl.BlockSpec(memory_space=pltpu.VMEM),
        scratch_shapes=[
            vmem((tiles, 2 * feat, LANES), BF16),
            vmem((hidden, feat), BF16),
            vmem((4, own_rows, feat), BF16),
            vmem((LANES, feat), BF16),
            vmem((LANES, feat), BF16),
            vmem((top, own_rows), jnp.int32),
            vmem((top, own_rows), F32),
            vmem((3, 8, LANES), F32),
            vmem((4, 8, LANES), F32),
            vmem((4 * pair, 2 * feat), BF16),
            vmem((2, pair, wide), F32),
            vmem((2, pair, wide), BF16),
            vmem((2, pair, wide), BF16),
            vmem((2, pair, wide // 2), F32),
            vmem((2, pair, wide // 2), BF16),
            vmem((2, pair, wide // 2), BF16),
            vmem((2, 2, own_rows, wide), BF16),
            vmem((2, pair, feat), F32),
            vmem((3, own_rows, feat), BF16),
            vmem((3, own_rows, feat), BF16),
            dma(chunk_count), dma(1), dma(5),
            dma(1), dma(3), dma(1), dma(3),
            *[dma(2, chunk_count) for _ in range(3)], dma(2, PIECE_OF[-1] + 1),
            dma(3), *[dma(1) for _ in range(6)],
            pltpu.SemaphoreType.REGULAR((3,)),
        ],
        compiler_params=pltpu.CompilerParams(
            collective_id=0, has_side_effects=True, vmem_limit_bytes=60 * 2**20
        ),
    )(
        tokens, gate_up_weight, down_weight, jnp.swapaxes(adapter_in, 1, 2), adapter_out,
        expert_ids.T, route_weight.T,
    )


def plain(tokens, gate_up_weight, down_weight, adapter_in, adapter_out, expert_ids, route_weight):
    exp_count = lax.axis_size("exp")
    own_rows, feat_width = tokens.shape
    all_tokens = lax.all_gather(tokens, "exp", axis=0, tiled=True)
    hidden_width = gate_up_weight.shape[2]
    pair_weight = gate_up_weight.reshape(feat_width, 2 * hidden_width)
    pair_share = lax.psum_scatter(
        jnp.dot(all_tokens, pair_weight, preferred_element_type=jnp.float32).astype(jnp.bfloat16),
        "tp",
        scatter_dimension=0,
        tiled=True,
    ).astype(jnp.float32)
    hidden_share = (
        jax.nn.silu(pair_share[:, :hidden_width]) * pair_share[:, hidden_width:]
    ).astype(jnp.bfloat16)
    hidden = lax.all_gather(hidden_share, "tp", axis=0, tiled=True)
    base_out = lax.psum_scatter(
        jnp.dot(hidden, down_weight, preferred_element_type=jnp.float32).astype(jnp.bfloat16),
        "exp",
        scatter_dimension=0,
        tiled=True,
    ).astype(jnp.float32)
    top_count = expert_ids.shape[1]
    expert_count = adapter_in.shape[0] * exp_count
    flat_ids = expert_ids.reshape(own_rows * top_count)
    flat_weight = route_weight.reshape(own_rows * top_count)
    expert_hits = (flat_ids[:, None] == jnp.arange(expert_count, dtype=jnp.int32)[None, :]).astype(
        jnp.int32
    )
    capacity = max(2, 2 * top_count * own_rows // expert_count)
    slot_index = jnp.sum((jnp.cumsum(expert_hits, axis=0) - expert_hits) * expert_hits, axis=1)
    slot_target = flat_ids * capacity + slot_index
    slot_hits = (
        slot_target[:, None] == jnp.arange(expert_count * capacity, dtype=jnp.int32)[None, :]
    )
    combine_matrix = jnp.sum(
        (slot_hits.astype(jnp.float32) * flat_weight[:, None]).reshape(
            own_rows, top_count, expert_count * capacity
        ),
        axis=1,
    )
    dispatch_matrix = slot_hits.T.astype(jnp.bfloat16)
    repeated = jnp.repeat(tokens, top_count, axis=0)
    outgoing = jnp.dot(dispatch_matrix, repeated, preferred_element_type=jnp.float32).astype(
        jnp.bfloat16
    )
    outgoing = outgoing.reshape(expert_count, capacity, feat_width)
    rank_partial = jnp.einsum(
        "scd,dr->scr",
        lax.all_to_all(outgoing, "exp", split_axis=0, concat_axis=0, tiled=True),
        adapter_in[0],
        preferred_element_type=jnp.float32,
    )
    rank_mid = lax.psum(rank_partial, "tp").astype(jnp.bfloat16)
    expert_out = jnp.einsum(
        "scr,rd->scd", rank_mid, adapter_out[0], preferred_element_type=jnp.float32
    ).astype(jnp.bfloat16)
    returned = lax.all_to_all(expert_out, "exp", split_axis=0, concat_axis=0, tiled=True)
    adapter_sum = jnp.dot(
        combine_matrix,
        returned.reshape(expert_count * capacity, feat_width).astype(jnp.float32),
        precision=lax.Precision.HIGHEST,
        preferred_element_type=jnp.float32,
    )
    return (base_out + adapter_sum).astype(jnp.bfloat16)


def local(tokens, gate_up_weight, *rest):
    own_rows, feat = tokens.shape
    fits = (
        lax.axis_size("tp") == 4
        and lax.axis_size("exp") == 4
        and rest[1].shape[0] == 1
        and rest[1].shape[2] <= LANES
        and own_rows % 16 == 0
        and feat % LANES == 0
        and gate_up_weight.shape[2] % (2 * LANES) == LANES
        and gate_up_weight.shape[2] >= 19 * LANES
    )
    return (fused if fits else plain)(tokens, gate_up_weight, *rest)


def solution(mesh):
    in_specs = (
        P(("grp", "exp"), "tp"),
        P("tp", None, "exp"),
        P("exp", "tp"),
        P("exp", "tp", None),
        P("exp", None, "tp"),
        P(("grp", "exp"), None),
        P(("grp", "exp"), None),
    )
    out_specs = P(("grp", "exp"), "tp")
    return jax.shard_map(local, mesh=mesh, in_specs=in_specs, out_specs=out_specs, check_vma=False)
```
